128 devices in a mesh: ctx: 32 (over z, x, core), exp: 4 (over y).
Axes of the slice: x: 4, y: 4, z: 4, core: 2. Of those that a mesh axis runs over, the one named last changes fastest.
Arguments:
- residual: bfloat16 [16384, 2048], P(('ctx', 'exp')), may hold values from -6 to 6
- mixed_qkv: bfloat16 [16384, 4096], P(('ctx', 'exp')), may hold values from -6 to 6
- output_gate: bfloat16 [16384, 2048], P(('ctx', 'exp')), may hold values from -6 to 6
- log_decay: float32 [16384, 16], P(('ctx', 'exp')), may hold values from -0.8 to 0, as said below
- write_strength: float32 [16384, 16], P(('ctx', 'exp')), may hold values from 0 to 1, as said below
- conv_weight: float32 [4, 4096], replicated, may hold values from -3 to 3
- norm_gain: float32 [128], replicated, may hold values from 0.1 to 1.9
- out_weight: bfloat16 [2048, 2048], P(None, 'exp'), may hold values from -0.125 to 0.125
- post_gain: float32 [2048], replicated, may hold values from 0.1 to 1.9
- router_weight: bfloat16 [2048, 256], replicated, may hold values from -0.125 to 0.125
- expert_ids: int32 [16384, 10], P(('ctx', 'exp')), may hold values from 0 to 255, all different within a row; in each aligned block of 128 rows (0 to 127, 128 to 255, ...) at most 6 rows name the same one
- expert_gate: bfloat16 [256, 2048, 512], P(('ctx', 'exp')), may hold values from -0.125 to 0.125
- expert_up: bfloat16 [256, 2048, 512], P(('ctx', 'exp')), may hold values from -0.125 to 0.125
- expert_down: bfloat16 [256, 512, 2048], P(('ctx', 'exp')), may hold values from -0.25 to 0.25
- shared_gate: bfloat16 [2048, 512], replicated, may hold values from -0.125 to 0.125
- shared_up: bfloat16 [2048, 512], replicated, may hold values from -0.125 to 0.125
- shared_down: bfloat16 [512, 2048], replicated, may hold values from -0.25 to 0.25
- shared_switch: bfloat16 [2048], replicated, may hold values from -0.125 to 0.125
Outputs:
- layer_out: bfloat16 [16384, 2048], P(('ctx', 'exp'))
The draws below stay inside these ranges and needn't reach their ends.
Inputs may be any that keep to these rules, and one draw needn't show every extreme that they name: `expert_ids`: in the 128 rows of one device no expert is named more than 6 times. `log_decay`: negative. `write_strength`: positive.
All inputs are finite; a program needn't handle non-finite values.
Results may differ from the reference program's by a relative error of at most 0.011.
Values may be sent and summed in bfloat16 or wider, within the bound.
A program may use at most 128 MiB of HBM per device.

```python
import math
import jax
import jax.numpy as jnp
import numpy as np
from jax import lax

D = 2048
VHEADS = 16
KHEADS = 8
HEAD = 128
FF = 512
SHARED_FF = 512
TOP = 10
SPAN = 64
TOK_DEV = 128
STREAM_LENGTH = 16384
EXPERTS = 256
CAP = 6


def head_plan(key):
    folded = jax.random.fold_in(key, 7)
    quick_heads = jax.random.uniform(folded, (VHEADS,)) < 0.5
    return quick_heads


def draw_log_decay(key, part):
    quick_heads = head_plan(key)
    stochastic_seeds = jax.random.split(jax.random.fold_in(key, 11), 6)
    quick_rates = jnp.exp(jax.random.uniform(stochastic_seeds[0], (VHEADS,), minval=jnp.log(1.0 / 50.0), maxval=jnp.log(1.0 / 30.0)))
    slow_rates = jnp.exp(jax.random.uniform(stochastic_seeds[1], (VHEADS,), minval=jnp.log(0.1), maxval=jnp.log(0.4))) / STREAM_LENGTH
    forgetting_speeds = jnp.where(quick_heads, quick_rates, slow_rates)
    jitter_scale = jax.random.uniform(stochastic_seeds[2], (STREAM_LENGTH, VHEADS), minval=0.5, maxval=1.5)
    segment_factor = jnp.exp(jax.random.uniform(stochastic_seeds[3], (STREAM_LENGTH // TOK_DEV, VHEADS), minval=jnp.log(0.5), maxval=jnp.log(2.0)))
    segment_factor = jnp.repeat(segment_factor, TOK_DEV, axis=0)
    spike_index = jax.random.randint(stochastic_seeds[4], (2,), 0, STREAM_LENGTH)
    magnitude_entries = jax.random.uniform(stochastic_seeds[5], (2, VHEADS), minval=0.22, maxval=0.69)
    element_index = jnp.arange(STREAM_LENGTH)[:, None]
    spike_indices = (element_index == spike_index[0]).astype(jnp.float32) * magnitude_entries[0][None, :]
    spike_indices = spike_indices + (element_index == spike_index[1]).astype(jnp.float32) * magnitude_entries[1][None, :]
    return (-(forgetting_speeds[None, :] * jitter_scale * segment_factor + spike_indices)).astype(jnp.float32)


def draw_write_strength(key, part):
    quick_heads = head_plan(key)
    stochastic_seeds = jax.random.split(jax.random.fold_in(key, 13), 3)
    quick_values = jax.random.uniform(stochastic_seeds[0], (STREAM_LENGTH, VHEADS), minval=0.05, maxval=0.95)
    slow_scale = jnp.exp(jax.random.uniform(stochastic_seeds[1], (VHEADS,), minval=jnp.log(0.25), maxval=0.0)) * HEAD / STREAM_LENGTH
    slow_values = slow_scale[None, :] * jax.random.uniform(stochastic_seeds[2], (STREAM_LENGTH, VHEADS), minval=0.5, maxval=1.5)
    return jnp.where(quick_heads[None, :], quick_values, slow_values).astype(jnp.float32)


def block_scale(key, dims, cuts, least, largest):
    factor_of, own = 1.0, jax.random.fold_in(key, 6)
    for dim, blocks in cuts:
        heights = jnp.exp(jax.random.uniform(jax.random.fold_in(own, dim), (blocks,), jnp.float32, least / len(cuts), largest / len(cuts)))
        factor_of = factor_of * jnp.repeat(heights, dims[dim] // blocks).reshape([-1 if axis == dim else 1 for axis in range(len(dims))])
    return factor_of


def assign_block(stream_key, own, number, rows, amount, top, bound, skew):
    order = jax.random.permutation(stream_key, amount)
    crowded, usual = portions_of(amount, rows * top, bound, skew, True), portions_of(amount, rows * top, bound, skew, False)
    places = jnp.arange(amount)

    def named(tallies, offset_by):
        used = int((tallies > 0).sum())
        fixed = max(1, used // 4)
        passed = fixed + (places - fixed + offset_by * (used - fixed)) % max(1, amount - fixed)
        return jnp.zeros((amount,), jnp.int32).at[order[jnp.where(places < fixed, places, passed)]].set(jnp.asarray(tallies, jnp.int32))

    tallies = jnp.where(number % 4 == 0, named(crowded, number // 4), named(usual, number - number // 4 - 1))
    mixed = jax.random.permutation(jax.random.fold_in(own, 3), amount)
    donor, receiver = mixed[0:amount // 2 * 2:2], mixed[1:amount // 2 * 2:2]
    room = jnp.minimum(tallies[donor] - 1, bound - tallies[receiver]) // 2
    room = jnp.where((donor == order[0]) | (receiver == order[0]) | (tallies[receiver] == 0), 0, jnp.maximum(room, 0))
    passed = jax.random.randint(jax.random.fold_in(own, 4), (amount // 2,), 0, 1 << 20) % (room + 1)
    tallies = tallies.at[donor].add(-passed).at[receiver].add(passed)
    items = jnp.searchsorted(jnp.cumsum(tallies), jnp.arange(rows * top), side="right").astype(jnp.int32)
    table = items.reshape(top, rows).T
    table = table[jax.random.permutation(jax.random.fold_in(own, 1), rows)]
    offset_by = jax.random.randint(jax.random.fold_in(own, 2), (rows, 1), 0, top)
    return jnp.take_along_axis(table, (jnp.arange(top)[None, :] + offset_by) % top, axis=1)


def portions_of(amount, total, reach, skew, full):
    loads = [(1 << 20) // math.isqrt(standing ** skew) + 1 for standing in range(1, amount + 1)]
    largest = reach if full else min(reach, max(-(-total // amount), total * loads[0] // sum(loads)))
    least = 1 if total - largest >= amount - 1 else 0
    counts, rest = [largest] + [least] * (amount - 1), total - largest - least * (amount - 1)
    while rest > 0:
        candidates = [i for i in range(1, amount) if counts[i] < largest] or [i for i in range(1, amount) if counts[i] < reach]
        pool, remaining = sum([loads[i] for i in candidates]), rest
        for i in candidates:
            more = min(reach - counts[i], max(1, remaining * loads[i] // pool), rest)
            counts[i] = counts[i] + more
            rest = rest - more
    return np.array(counts)


def normal_values(own_key, shape, deviation, bound, shards=(), kind=jnp.bfloat16):
    result = deviation * jax.random.normal(own_key, shape, jnp.float32)
    if shards:
        result = result * block_scale(own_key, shape, shards, -0.22, 0.18)
    return jnp.clip(result, -bound, bound).astype(kind)


def setup_inputs(seed: int = 0) -> dict:
    splits = jax.random.split(jax.random.key(seed), 19)
    residual = normal_values(splits[0], (STREAM_LENGTH, D), 1.0, 6.0, ((0, 128),))
    mixed_qkv = normal_values(splits[1], (STREAM_LENGTH, (2 * KHEADS + VHEADS) * HEAD), 1.0, 6.0, ((0, 128),))
    output_gate = normal_values(splits[2], (STREAM_LENGTH, VHEADS * HEAD), 1.0, 6.0, ((0, 128),))
    log_decay = draw_log_decay(jax.random.fold_in(splits[18], 71), 0)
    write_strength = draw_write_strength(jax.random.fold_in(splits[18], 71), 0)
    conv_weight = normal_values(splits[5], (4, (2 * KHEADS + VHEADS) * HEAD), 0.5, 3.0, (), jnp.float32)
    norm_gain = jnp.clip(1.0 + 0.18 * jax.random.normal(splits[6], (HEAD,), jnp.float32), 0.1, 1.9)
    out_weight = normal_values(splits[7], (VHEADS * HEAD, D), (VHEADS * HEAD) ** -0.5, 0.125, ((1, 4),))
    post_gain = jnp.clip(1.0 + 0.18 * jax.random.normal(splits[8], (D,), jnp.float32), 0.1, 1.9)
    router_weight = normal_values(splits[9], (D, EXPERTS), D ** -0.5, 0.125)
    expert_ids_keys = jax.random.split(jax.random.fold_in(splits[10], 1), STREAM_LENGTH // TOK_DEV)
    expert_ids_turns = jax.random.permutation(jax.random.fold_in(splits[10], 3), STREAM_LENGTH // TOK_DEV)
    expert_ids = jax.vmap(lambda own, number: assign_block(jax.random.fold_in(splits[10], 2), own, number, TOK_DEV, EXPERTS, TOP, CAP, 1))(expert_ids_keys, expert_ids_turns).reshape((STREAM_LENGTH, TOP))
    expert_gate = normal_values(splits[11], (EXPERTS, D, FF), D ** -0.5, 0.125, ((0, 128),))
    expert_up = normal_values(splits[12], (EXPERTS, D, FF), D ** -0.5, 0.125, ((0, 128),))
    expert_down = normal_values(splits[13], (EXPERTS, FF, D), FF ** -0.5, 0.25, ((0, 128),))
    shared_gate = normal_values(splits[14], (D, SHARED_FF), D ** -0.5, 0.125)
    shared_up = normal_values(splits[15], (D, SHARED_FF), D ** -0.5, 0.125)
    shared_down = normal_values(splits[16], (SHARED_FF, D), SHARED_FF ** -0.5, 0.25)
    shared_switch = normal_values(splits[17], (D,), D ** -0.5, 0.125)
    return dict(residual=residual, mixed_qkv=mixed_qkv, output_gate=output_gate, log_decay=log_decay, write_strength=write_strength, conv_weight=conv_weight, norm_gain=norm_gain, out_weight=out_weight, post_gain=post_gain, router_weight=router_weight, expert_ids=expert_ids, expert_gate=expert_gate, expert_up=expert_up, expert_down=expert_down, shared_gate=shared_gate, shared_up=shared_up, shared_down=shared_down, shared_switch=shared_switch)


highest_precision = lax.Precision.HIGHEST
epsilon = 1e-06

def short_conv(mixed_qkv, conv_weight, before):
    row_count = mixed_qkv.shape[0]
    padded = jnp.concatenate([before, mixed_qkv], axis=0).astype(jnp.float32)
    summed = conv_weight[3] * padded[3:3 + row_count]
    for tap_index in range(3):
        summed = summed + conv_weight[tap_index] * padded[tap_index:tap_index + row_count]
    return jax.nn.silu(summed)

def unit_rows(values_in):
    return values_in * lax.rsqrt(lax.optimization_barrier(jnp.sum(values_in * values_in, axis=-1, keepdims=True)) + epsilon)

def prepare(mixed_qkv, conv_weight, before):
    activated = short_conv(mixed_qkv, conv_weight, before)
    row_count = activated.shape[0]
    key_width = KHEADS * HEAD
    query_rows = unit_rows(activated[:, :key_width].reshape(row_count, KHEADS, HEAD)) * HEAD ** (-0.5)
    key_rows = unit_rows(activated[:, key_width:2 * key_width].reshape(row_count, KHEADS, HEAD))
    value_rows = activated[:, 2 * key_width:].reshape(row_count, VHEADS, HEAD)
    per_group = VHEADS // KHEADS
    query_rows = jnp.repeat(query_rows, per_group, axis=1)
    key_rows = jnp.repeat(key_rows, per_group, axis=1)
    return (query_rows.transpose(1, 0, 2), key_rows.transpose(1, 0, 2), value_rows.transpose(1, 0, 2))

def to_spans(head_rows):
    head_count, row_count, inner_width = head_rows.shape
    return head_rows.reshape(head_count, row_count // SPAN, SPAN, inner_width).transpose(1, 0, 2, 3)

def rates_to_spans(token_rates):
    row_count, head_count = token_rates.shape
    return token_rates.T.reshape(head_count, row_count // SPAN, SPAN).transpose(1, 0, 2)

def span_terms(query_rows, key_rows, value_rows, decay_rows, strength_rows):
    length = query_rows.shape[1]
    inner_width = key_rows.shape[2]
    cumul = jnp.cumsum(decay_rows, axis=1)
    causal = jnp.arange(length, dtype=jnp.int32)[:, None] >= jnp.arange(length, dtype=jnp.int32)[None, :]
    strict = jnp.arange(length, dtype=jnp.int32)[:, None] > jnp.arange(length, dtype=jnp.int32)[None, :]
    log_gap = cumul[:, :, None] - cumul[:, None, :]
    ratios = jnp.where(causal, jnp.exp(jnp.where(causal, log_gap, 0.0)), 0.0)
    key_inner = jnp.einsum('hck,hsk->hcs', key_rows, key_rows, precision=highest_precision)
    lower_part = jnp.where(strict, ratios * key_inner, 0.0) * strength_rows[:, :, None]
    system = jnp.eye(length, dtype=jnp.float32)[None] + lower_part
    decays = jnp.exp(cumul)
    right_operand = jnp.concatenate([strength_rows[:, :, None] * decays[:, :, None] * key_rows, strength_rows[:, :, None] * value_rows], axis=2)
    solved = jax.scipy.linalg.solve_triangular(system, right_operand, lower=True, unit_diagonal=True)
    key_weights = solved[:, :, :inner_width]
    fresh_values = solved[:, :, inner_width:]
    to_end = jnp.exp(cumul[:, -1:] - cumul)
    decayed_state = key_rows * to_end[:, :, None]
    identity = jnp.eye(inner_width, dtype=jnp.float32)[None]
    carry_transform = jnp.exp(cumul[:, -1])[:, None, None] * identity - jnp.einsum('hck,hcj->hkj', decayed_state, key_weights, precision=highest_precision)
    carry_offset = jnp.einsum('nae,nap->nep', decayed_state, fresh_values, precision=highest_precision)
    scores = jnp.einsum('hck,hsk->hcs', query_rows, key_rows, precision=highest_precision) * ratios
    read_transform = query_rows * decays[:, :, None] - jnp.einsum('hcs,hsk->hck', scores, key_weights, precision=highest_precision)
    read_offset = jnp.einsum('hcs,hsv->hcv', scores, fresh_values, precision=highest_precision)
    return (carry_transform, carry_offset, read_transform, read_offset)

def reference(residual, mixed_qkv, output_gate, log_decay, write_strength, conv_weight, norm_gain, out_weight, post_gain, router_weight, expert_ids, expert_gate, expert_up, expert_down, shared_gate, shared_up, shared_down, shared_switch):
    padding = jnp.zeros((3, mixed_qkv.shape[1]), mixed_qkv.dtype)
    query_rows, key_rows, value_rows = prepare(mixed_qkv, conv_weight, padding)
    span_inputs = (to_spans(query_rows), to_spans(key_rows), to_spans(value_rows), rates_to_spans(log_decay), rates_to_spans(write_strength))

    def advance(current_state, pieces):
        carry_transform, carry_offset, read_transform, read_offset = span_terms(*pieces)
        produced_output = jnp.einsum('urm,umn->urn', read_transform, current_state, precision=highest_precision) + read_offset
        following_state = jnp.einsum('coq,cqd->cod', carry_transform, current_state, precision=highest_precision) + carry_offset
        return (following_state, produced_output)
    start_state = jnp.zeros((VHEADS, HEAD, HEAD), jnp.float32)
    _, produced_output = lax.scan(advance, start_state, span_inputs)
    mixer_out = produced_output.transpose(0, 2, 1, 3).reshape(STREAM_LENGTH, VHEADS, HEAD)
    gate_rows = output_gate.reshape(STREAM_LENGTH, VHEADS, HEAD).astype(jnp.float32)
    normed = mixer_out * lax.rsqrt(lax.optimization_barrier(jnp.mean(mixer_out * mixer_out, axis=-1, keepdims=True)) + epsilon)
    normed = (normed * norm_gain * jax.nn.silu(gate_rows)).reshape(STREAM_LENGTH, VHEADS * HEAD).astype(jnp.bfloat16)
    after_mix = (residual.astype(jnp.float32) + jnp.dot(normed.astype(jnp.float32), out_weight.astype(jnp.float32), preferred_element_type=jnp.float32)).astype(jnp.bfloat16)
    after_wide = after_mix.astype(jnp.float32)
    routed_in = (after_wide * lax.rsqrt(lax.optimization_barrier(jnp.mean(after_wide * after_wide, axis=-1, keepdims=True)) + epsilon) * post_gain).astype(jnp.bfloat16)
    logits = jnp.dot(routed_in.astype(jnp.float32), router_weight.astype(jnp.float32), preferred_element_type=jnp.float32)
    chosen = jnp.exp(jnp.take_along_axis(logits, expert_ids, axis=1))
    gate_weights = chosen / lax.optimization_barrier(jnp.sum(chosen, axis=1, keepdims=True))
    shared_hidden = (jax.nn.silu(jnp.dot(routed_in.astype(jnp.float32), shared_gate.astype(jnp.float32), preferred_element_type=jnp.float32)) * jnp.dot(routed_in.astype(jnp.float32), shared_up.astype(jnp.float32), preferred_element_type=jnp.float32)).astype(jnp.bfloat16)
    switch_rows = jax.nn.sigmoid(jnp.dot(routed_in.astype(jnp.float32), shared_switch.astype(jnp.float32), preferred_element_type=jnp.float32))
    shared_out = switch_rows[:, None] * jnp.dot(shared_hidden.astype(jnp.float32), shared_down.astype(jnp.float32), preferred_element_type=jnp.float32)
    block_count = STREAM_LENGTH // TOK_DEV
    flat_ids = expert_ids.reshape(block_count, TOK_DEV * TOP)

    def ranks_of(row_ids):
        onehot = (row_ids[:, None] == jnp.arange(EXPERTS, dtype=jnp.int32)[None, :]).astype(jnp.int32)
        earlier = jnp.cumsum(onehot, axis=0) - onehot
        return lax.optimization_barrier(jnp.sum(earlier * onehot, axis=1)).astype(jnp.int32)
    slot_rank = lax.map(ranks_of, flat_ids)
    block_of = jnp.broadcast_to(jnp.arange(block_count, dtype=jnp.int32)[:, None], flat_ids.shape)
    token_of = block_of * TOK_DEV + jnp.arange(TOK_DEV * TOP, dtype=jnp.int32)[None, :] // TOP
    rows_table = jnp.zeros((EXPERTS, block_count, CAP), jnp.int32).at[flat_ids, block_of, slot_rank].set(token_of)
    scale_table = jnp.zeros((EXPERTS, block_count, CAP), jnp.float32).at[flat_ids, block_of, slot_rank].set(gate_weights.reshape(block_count, TOK_DEV * TOP))

    def expert_step(accumulated, pieces):
        row_ids, slot_scale, gate_w, up_w, down_w = pieces
        row_ids = row_ids.reshape(-1)
        slot_scale = slot_scale.reshape(-1)
        taken_rows = routed_in[row_ids]
        expert_hidden = (jax.nn.silu(jnp.dot(taken_rows.astype(jnp.float32), gate_w.astype(jnp.float32), preferred_element_type=jnp.float32)) * jnp.dot(taken_rows.astype(jnp.float32), up_w.astype(jnp.float32), preferred_element_type=jnp.float32)).astype(jnp.bfloat16)
        expert_out = jnp.dot(expert_hidden.astype(jnp.float32), down_w.astype(jnp.float32), preferred_element_type=jnp.float32).astype(jnp.bfloat16)
        return (accumulated.at[row_ids].add(expert_out.astype(jnp.float32) * slot_scale[:, None]), None)
    routed, _ = lax.scan(expert_step, jnp.zeros((STREAM_LENGTH, D), jnp.float32), (rows_table, scale_table, expert_gate, expert_up, expert_down))
    return (after_mix.astype(jnp.float32) + routed + shared_out).astype(jnp.bfloat16)
```

```python
import jax
import jax.numpy as jnp
import numpy as np
from jax import lax
from jax.experimental import pallas as pl
from jax.experimental.pallas import tpu as pltpu
from jax.sharding import Mesh
from jax.sharding import PartitionSpec as P

VHEADS = 16
HEAD = 128
ROWS = 128
TOP = 10
CAP = 6
WIDTH = 2048
EXPERTS = 256
AXES = ("ctx_0", "ctx_1", "ctx_2", "exp")
SAME_CORE = ("ctx_0", "ctx_1", "exp")
PEERS = 64
SLOTS = 4 * CAP
SENT = PEERS * SLOTS
BATCH = 8
MESH = pl.DeviceIdType.MESH
epsilon = 1e-06
F32 = jnp.float32
BF16 = jnp.bfloat16
VM = pl.BlockSpec(memory_space=pltpu.VMEM)
ANY = pl.BlockSpec(memory_space=pl.ANY)


def nn(a, b):
    return lax.dot_general(a, b, (((1,), (0,)), ((), ())), preferred_element_type=F32)


def nt(a, b):
    return lax.dot_general(a, b, (((1,), (1,)), ((), ())), preferred_element_type=F32)


def tn(a, b):
    return lax.dot_general(a, b, (((0,), (0,)), ((), ())), preferred_element_type=F32)


def silu(v):
    return v / (1.0 + jnp.exp(-v))


def local_kernel(
    q_ref, k_ref, v_ref, qb_ref, kb_ref, vb_ref, qw_ref, kw_ref, vw_ref, ld_ref, ws_ref,
    maps_ref, reads_ref, offs_ref, pad, cumt, lows, inv,
):
    first = pl.program_id(0) * BATCH
    rows = lax.broadcasted_iota(jnp.int32, (ROWS, ROWS), 0)
    cols = lax.broadcasted_iota(jnp.int32, (ROWS, ROWS), 1)
    causal = rows >= cols
    strict = rows > cols
    ones = causal.astype(F32)
    decay = ld_ref[...]
    highest = lax.Precision.HIGHEST
    cum = lax.dot_general(
        ones, decay, (((1,), (0,)), ((), ())), precision=highest, preferred_element_type=F32
    )
    cumt[...] = lax.dot_general(
        decay, ones, (((0,), (1,)), ((), ())), precision=highest, preferred_element_type=F32
    )
    strength = ws_ref[...]
    lane = lax.broadcasted_iota(jnp.int32, (ROWS, VHEADS), 1)

    def column(table, head):
        return jnp.sum(jnp.where(lane == head, table, 0.0), axis=1, keepdims=True)

    def activated(x_ref, b_ref, w_ref):
        n = x_ref.shape[1]
        pad[0:8, 0:n] = b_ref[...].astype(F32)
        pad[8 : 8 + ROWS, 0:n] = x_ref[...].astype(F32)
        total = w_ref[3:4, :] * pad[8 : 8 + ROWS, 0:n]
        for tap in range(3):
            total = total + w_ref[tap : tap + 1, :] * pad[5 + tap : 5 + tap + ROWS, 0:n]
        return silu(total)

    def unit(a):
        return a * lax.rsqrt(jnp.sum(a * a, axis=-1, keepdims=True) + epsilon)

    queries = activated(q_ref, qb_ref, qw_ref)
    keys = activated(k_ref, kb_ref, kw_ref)
    values = activated(v_ref, vb_ref, vw_ref)
    eye = (rows == cols).astype(F32)
    per_head = []
    for pair in range(BATCH // 2):
        part = slice(pair * HEAD, (pair + 1) * HEAD)
        query = unit(queries[:, part]) * HEAD ** (-0.5)
        key = unit(keys[:, part])
        key_b = key.astype(BF16)
        inner = nt(key_b, key_b)
        scores = nt(query.astype(BF16), key_b)
        for i in (2 * pair, 2 * pair + 1):
            c = column(cum, first + i)
            b = column(strength, first + i)
            gap = c - cumt[pl.ds(first + i, 1), :]
            ratios = jnp.where(causal, jnp.exp(jnp.where(causal, gap, 0.0)), 0.0)
            low = jnp.where(strict, ratios * inner, 0.0) * b
            lows[i] = low
            inv[i] = eye - jnp.where((rows >> 1) == (cols >> 1), low, 0.0)
            last = c[ROWS - 1 : ROWS, :]
            decays = jnp.exp(c)
            right = jnp.concatenate(
                [(b * decays * key).astype(BF16), (b * values[:, i * HEAD : (i + 1) * HEAD]).astype(BF16)],
                axis=1,
            )
            per_head.append(
                (
                    (scores * ratios).astype(BF16),
                    query * decays,
                    (key * jnp.exp(last - c)).astype(BF16),
                    right,
                    jnp.exp(last) - 1.0,
                )
            )
    for level in range(1, 7):
        here = ((rows >> (level + 1)) == (cols >> (level + 1))) & ((rows >> level) != (cols >> level))
        for i in range(BATCH):
            x = inv[i]
            x_b = x.astype(BF16)
            off = jnp.where(here, lows[i], 0.0).astype(BF16)
            inv[i] = x - nn(x_b, nn(off, x_b).astype(BF16))
    for i in range(BATCH):
        score, read, end_key, right, less = per_head[i]
        solved = nn(inv[i].astype(BF16), right).astype(BF16)
        carried = tn(solved, end_key)
        maps_ref[i, 0:HEAD, :] = (less * eye - carried[0:HEAD]).astype(BF16)
        maps_ref[i, HEAD : 2 * HEAD, :] = carried[HEAD:].astype(BF16)
        produced = nn(score, solved)
        reads_ref[i] = (read - produced[:, 0:HEAD]).astype(BF16)
        offs_ref[i] = produced[:, HEAD:]


def local_terms(mixed, before, conv_weight, log_decay, write_strength):
    n = BATCH // 2 * HEAD
    steps = VHEADS // BATCH

    def wide(rows_of, width, base):
        return pl.BlockSpec((rows_of, width), lambda s: (0, base + s))

    def three(rows_of):
        return [wide(rows_of, n, 0), wide(rows_of, n, steps), wide(rows_of, 2 * n, steps)]

    whole = pl.BlockSpec((ROWS, VHEADS), lambda s: (0, 0))
    return pl.pallas_call(
        local_kernel,
        name="local_terms",
        grid=(steps,),
        in_specs=three(ROWS) + three(8) + three(4) + [whole, whole],
        out_specs=[
            pl.BlockSpec((BATCH, 2 * HEAD, HEAD), lambda s: (s, 0, 0)),
            pl.BlockSpec((BATCH, ROWS, HEAD), lambda s: (s, 0, 0)),
            pl.BlockSpec((BATCH, ROWS, HEAD), lambda s: (s, 0, 0)),
        ],
        out_shape=[
            jax.ShapeDtypeStruct((VHEADS, 2 * HEAD, HEAD), BF16),
            jax.ShapeDtypeStruct((VHEADS, ROWS, HEAD), BF16),
            jax.ShapeDtypeStruct((VHEADS, ROWS, HEAD), F32),
        ],
        scratch_shapes=[
            pltpu.VMEM((8 + ROWS, 2 * n), F32),
            pltpu.VMEM((VHEADS, ROWS), F32),
            pltpu.VMEM((BATCH, ROWS, ROWS), F32),
            pltpu.VMEM((BATCH, ROWS, ROWS), F32),
        ],
        compiler_params=pltpu.CompilerParams(vmem_limit_bytes=40 << 20),
        cost_estimate=pl.CostEstimate(
            flops=8_000_000_000, bytes_accessed=6_000_000, transcendentals=1_000_000
        ),
    )(
        mixed, mixed, mixed, before, before, before, conv_weight, conv_weight, conv_weight,
        log_decay, write_strength,
    )


def scan_kernel(
    maps, starts, got1, pre1, tot1, got2, pre2, tot2, got3, st4, got4, st5, got5,
    send1, recv1, send2, recv2, send3, recv3, send4, recv4, send5, recv5,
):
    z, x, c, y = (lax.axis_index(a) for a in AXES)
    place = 2 * x + c
    barrier = pltpu.get_barrier_semaphore()

    def at(j, axis):
        if axis == "y":
            return {"exp": lax.rem(y + j, 4)}
        if axis == "z":
            return {"ctx_0": lax.rem(z + j, 4)}
        other = lax.rem(place + j, 8)
        return {"ctx_1": other // 2, "ctx_2": lax.rem(other, 2)}

    for axis, count in (("y", 4), ("z", 4), ("p", 8)):
        for j in range(1, count):
            pl.semaphore_signal(barrier, inc=1, device_id=at(j, axis), device_id_type=MESH)
    pl.semaphore_wait(barrier, 13)
    started = []

    def send(src, dst, s, r, device):
        copy = pltpu.make_async_remote_copy(
            src_ref=src, dst_ref=dst, send_sem=s, recv_sem=r, device_id=device, device_id_type=MESH
        )
        copy.start()
        started.append(copy)
        return copy

    copies = []
    for j in range(1, 4):
        other = lax.rem(y + j, 4)
        copies.append(
            send(maps.at[pl.ds(4 * other, 4)], got1.at[y], send1.at[j], recv1.at[j], at(j, "y"))
        )
    got1[y] = maps[pl.ds(4 * y, 4)]
    for copy in copies:
        copy.wait_recv()
    for h in range(4):
        run = got1[0, h].astype(F32)
        for m in range(1, 4):
            pre1[m - 1, h] = run.astype(BF16)
            run = run + got1[m, h].astype(F32) + nn(run.astype(BF16), got1[m, h, 0:HEAD, :])
        tot1[h] = run.astype(BF16)

    copies = []
    for j in range(1, 8):
        other = lax.rem(place + j, 8)
        head, half = other // 2, lax.rem(other, 2)
        copies.append(
            send(
                tot1.at[head, 0:HEAD], got2.at[place, 0:HEAD], send2.at[j, 0], recv2.at[j, 0],
                at(j, "p"),
            )
        )
        copies.append(
            send(
                tot1.at[head, pl.ds(pl.multiple_of(HEAD + 64 * half, 64), 64)],
                got2.at[place, HEAD : HEAD + 64],
                send2.at[j, 1], recv2.at[j, 1], at(j, "p"),
            )
        )
    got2[place, 0:HEAD, :] = tot1[x, 0:HEAD, :]
    got2[place, HEAD : HEAD + 64, :] = tot1[x, pl.ds(pl.multiple_of(HEAD + 64 * c, 64), 64), :]
    for copy in copies:
        copy.wait_recv()
    run = got2[0].astype(F32)
    for p in range(1, 8):
        pre2[p - 1] = run.astype(BF16)
        run = run + got2[p].astype(F32) + nn(run.astype(BF16), got2[p, 0:HEAD, :])
    tot2[...] = run.astype(BF16)

    copies = []
    for j in range(1, 4):
        copies.append(send(tot2, got3.at[z], send3.at[j], recv3.at[j], at(j, "z")))
    got3[z] = tot2[...]
    for copy in copies:
        copy.wait_recv()
    state = jnp.zeros((64, HEAD), F32)
    for k in range(3):
        later = state + got3[k, HEAD:, :].astype(F32) + nn(state.astype(BF16), got3[k, 0:HEAD, :])
        state = jnp.where(k < z, later, state)
    state_b = state.astype(BF16)
    st4[0] = state_b
    for p in range(1, 8):
        st4[p] = (
            state + pre2[p - 1, HEAD:, :].astype(F32) + nn(state_b, pre2[p - 1, 0:HEAD, :])
        ).astype(BF16)

    copies = []
    rows_here = pl.ds(pl.multiple_of(64 * c, 64), 64)
    for j in range(1, 8):
        other = lax.rem(place + j, 8)
        copies.append(
            send(st4.at[other], got4.at[x, rows_here], send4.at[j], recv4.at[j], at(j, "p"))
        )
    got4[x, rows_here, :] = st4[place]
    for copy in copies:
        copy.wait_recv()
    for h in range(4):
        begin = got4[h]
        st5[0, h] = begin
        for m in range(1, 4):
            st5[m, h] = (
                begin.astype(F32)
                + pre1[m - 1, h, HEAD:, :].astype(F32)
                + nn(begin, pre1[m - 1, h, 0:HEAD, :])
            ).astype(BF16)

    copies = []
    for j in range(1, 4):
        other = lax.rem(y + j, 4)
        copies.append(send(st5.at[other], got5.at[y], send5.at[j], recv5.at[j], at(j, "y")))
    got5[y] = st5[y]
    for copy in copies:
        copy.wait_recv()
    for m in range(4):
        starts[4 * m : 4 * m + 4] = got5[m]
    for copy in started:
        copy.wait_send()


def scan_states(maps):
    dma = pltpu.SemaphoreType.DMA
    return pl.pallas_call(
        scan_kernel,
        name="scan_states",
        in_specs=[VM],
        out_specs=VM,
        out_shape=jax.ShapeDtypeStruct((VHEADS, HEAD, HEAD), BF16),
        scratch_shapes=[
            pltpu.VMEM((4, 4, 2 * HEAD, HEAD), BF16),
            pltpu.VMEM((3, 4, 2 * HEAD, HEAD), BF16),
            pltpu.VMEM((4, 2 * HEAD, HEAD), BF16),
            pltpu.VMEM((8, HEAD + 64, HEAD), BF16),
            pltpu.VMEM((7, HEAD + 64, HEAD), BF16),
            pltpu.VMEM((HEAD + 64, HEAD), BF16),
            pltpu.VMEM((4, HEAD + 64, HEAD), BF16),
            pltpu.VMEM((8, 64, HEAD), BF16),
            pltpu.VMEM((4, HEAD, HEAD), BF16),
            pltpu.VMEM((4, 4, HEAD, HEAD), BF16),
            pltpu.VMEM((4, 4, HEAD, HEAD), BF16),
            dma((4,)), dma((4,)), dma((8, 2)), dma((8, 2)), dma((4,)), dma((4,)),
            dma((8,)), dma((8,)), dma((4,)), dma((4,)),
        ],
        compiler_params=pltpu.CompilerParams(
            collective_id=0, has_side_effects=True, vmem_limit_bytes=32 << 20
        ),
        cost_estimate=pl.CostEstimate(
            flops=30_000_000_000, bytes_accessed=4_000_000, transcendentals=0
        ),
    )(maps)


def mix_kernel(
    reads, offs, starts, gate_ref, gain_ref, res_ref, post_ref, own, a1, a2, a3, b1, b2, b3,
    after_ref, routed_ref, weights, normed, total, sems,
):
    c, y = lax.axis_index("ctx_2"), lax.axis_index("exp")
    half = WIDTH // 2
    mine = pl.ds(pl.multiple_of(half * c, half), half)
    theirs = pl.ds(pl.multiple_of(half * (1 - c), half), half)
    loads = [[pltpu.make_async_copy(own, weights.at[0], sems.at[0])]]
    for j, (a, b) in enumerate(((a1, b1), (a2, b2), (a3, b3)), 1):
        loads.append(
            [
                pltpu.make_async_copy(a, weights.at[j, mine], sems.at[2 * j - 1]),
                pltpu.make_async_copy(b, weights.at[j, theirs], sems.at[2 * j]),
            ]
        )
    for group in loads:
        for load in group:
            load.start()
    gain = gain_ref[...]
    for h in range(VHEADS):
        part = slice(h * HEAD, (h + 1) * HEAD)
        out = offs[h] + nt(reads[h], starts[h])
        out = out * lax.rsqrt(jnp.mean(out * out, axis=-1, keepdims=True) + epsilon)
        normed[:, part] = (out * gain * silu(gate_ref[:, part].astype(F32))).astype(BF16)
    columns = WIDTH // 4
    for j in range(4):
        for load in loads[j]:
            load.wait()
        block = lax.rem(y + 4 - j, 4)
        here = pl.ds(pl.multiple_of(columns * block, columns), columns)
        total[:, here] = nn(normed[...], weights[j])
    after = (res_ref[...].astype(F32) + total[...]).astype(BF16)
    after_ref[...] = after
    wide = after.astype(F32)
    routed_ref[...] = (
        wide * lax.rsqrt(jnp.mean(wide * wide, axis=-1, keepdims=True) + epsilon) * post_ref[...]
    ).astype(BF16)


def mix(reads, offs, starts, gate, gain, residual, post, own, near, far):
    shape = jax.ShapeDtypeStruct((ROWS, WIDTH), BF16)
    return pl.pallas_call(
        mix_kernel,
        name="mix",
        in_specs=[VM] * 7 + [ANY] * 7,
        out_specs=[VM, VM],
        out_shape=[shape, shape],
        scratch_shapes=[
            pltpu.VMEM((4, WIDTH, WIDTH // 4), BF16),
            pltpu.VMEM((ROWS, WIDTH), BF16),
            pltpu.VMEM((ROWS, WIDTH), F32),
            pltpu.SemaphoreType.DMA((7,)),
        ],
        compiler_params=pltpu.CompilerParams(vmem_limit_bytes=40 << 20),
        cost_estimate=pl.CostEstimate(
            flops=2_000_000_000, bytes_accessed=12_000_000, transcendentals=300_000
        ),
    )(reads, offs, starts, gate, gain, residual, post, own, *near, *far)


LANES = np.arange(SENT)
PEER, INSIDE = LANES // SLOTS, LANES % SLOTS
EXPERT_OF = 2 * (PEER // 4 * 8 + PEER % 4) + INSIDE // (2 * CAP)
TABLE = np.stack(
    [EXPERT_OF, INSIDE % (2 * CAP) // CAP, INSIDE % CAP] + [np.zeros(SENT, np.int64)] * 5
).astype(np.int32)


def slot_kernel(ids_ref, table_ref, sel_ref):
    c = lax.axis_index("ctx_2")
    wanted = table_ref[0:1, :] + 8 * c
    source, slot = table_ref[1:2, :], table_ref[2:3, :]
    rows = lax.broadcasted_iota(jnp.int32, (ROWS, ROWS), 0)
    cols = lax.broadcasted_iota(jnp.int32, (ROWS, ROWS), 1)
    earlier = (rows > cols).astype(BF16)
    for half in range(2):
        part = slice(half * ROWS, (half + 1) * ROWS)
        ids = ids_ref[part, :]
        hit = (ids[:, 0:1] == wanted) & (source == half)
        for k in range(1, TOP):
            hit = hit | ((ids[:, k : k + 1] == wanted) & (source == half))
        marks = hit.astype(F32)
        rank = nn(earlier, marks.astype(BF16))
        sel_ref[part, :] = jnp.where(rank == slot.astype(F32), marks, 0.0).astype(BF16)


def slots(ids):
    return pl.pallas_call(
        slot_kernel,
        name="slots",
        in_specs=[VM, VM],
        out_specs=VM,
        out_shape=jax.ShapeDtypeStruct((2 * ROWS, SENT), BF16),
        compiler_params=pltpu.CompilerParams(vmem_limit_bytes=32 << 20),
        cost_estimate=pl.CostEstimate(
            flops=200_000_000, bytes_accessed=1_000_000, transcendentals=0
        ),
    )(ids, jnp.asarray(TABLE))


def send_kernel(own, other, sel_ref, ids_ref, table_ref, router, out_ref, high_ref, low_ref):
    rows = jnp.concatenate([own[...], other[...]], axis=0)

    @pl.when(pl.program_id(0) == 0)
    def _():
        logits = nn(rows, router[...])
        lane = lax.broadcasted_iota(jnp.int32, (2 * ROWS, EXPERTS), 1)
        ids = ids_ref[...]
        hit = ids[:, 0:1] == lane
        for k in range(1, TOP):
            hit = hit | (ids[:, k : k + 1] == lane)
        chosen = jnp.where(hit, jnp.exp(jnp.where(hit, logits, 0.0)), 0.0)
        gates = chosen / jnp.sum(chosen, axis=1, keepdims=True)
        wanted = table_ref[0:1, :] + 8 * lax.axis_index("ctx_2")
        spread = (
            lax.broadcasted_iota(jnp.int32, (EXPERTS, SENT), 0) == wanted
        ).astype(BF16)
        high = gates.astype(BF16)
        low = (gates - high.astype(F32)).astype(BF16)
        sel = sel_ref[...]
        high_ref[...] = nn(high, spread).astype(BF16) * sel
        low_ref[...] = nn(low, spread).astype(BF16) * sel

    n = out_ref.shape[1]
    here = pl.ds(pl.multiple_of(pl.program_id(0) * n, n), n)
    cut = jnp.concatenate([own[:, here], other[:, here]], axis=0)
    out_ref[...] = tn(sel_ref[...], cut).astype(BF16)


def to_send(own, other, sel, ids, router):
    n = 256
    full = lambda *shape: pl.BlockSpec(shape, lambda s: (0,) * len(shape))
    return pl.pallas_call(
        send_kernel,
        name="to_send",
        grid=(WIDTH // n,),
        in_specs=[
            full(ROWS, WIDTH), full(ROWS, WIDTH), full(2 * ROWS, SENT), full(2 * ROWS, TOP),
            full(8, SENT), full(WIDTH, EXPERTS),
        ],
        out_specs=[
            pl.BlockSpec((SENT, n), lambda s: (0, s)), full(2 * ROWS, SENT), full(2 * ROWS, SENT),
        ],
        out_shape=[
            jax.ShapeDtypeStruct((SENT, WIDTH), BF16),
            jax.ShapeDtypeStruct((2 * ROWS, SENT), BF16),
            jax.ShapeDtypeStruct((2 * ROWS, SENT), BF16),
        ],
        compiler_params=pltpu.CompilerParams(vmem_limit_bytes=40 << 20),
        cost_estimate=pl.CostEstimate(
            flops=2_000_000_000, bytes_accessed=10_000_000, transcendentals=70_000
        ),
    )(own, other, sel, ids, jnp.asarray(TABLE), router)


def expert_kernel(x_ref, gate_ref, up_ref, down_ref, out_ref):
    x = x_ref[...]
    n = x.shape[0]
    inside = lax.rem(lax.broadcasted_iota(jnp.int32, (n, 1), 0), SLOTS)
    total = None
    for e in range(2):
        hidden = silu(nn(x, gate_ref[e])) * nn(x, up_ref[e])
        hidden = jnp.where((inside >= 2 * CAP) == bool(e), hidden, 0.0).astype(BF16)
        part = nn(hidden, down_ref[e])
        total = part if total is None else total + part
    out_ref[...] = total.astype(BF16)


def run_experts(received, gate, up, down):
    n = SENT // 8
    once = lambda a: pl.BlockSpec(a.shape, lambda s: (0, 0, 0), pipeline_mode=pl.Buffered(1))
    rows = pl.BlockSpec((n, WIDTH), lambda s: (s, 0))
    return pl.pallas_call(
        expert_kernel,
        name="experts",
        grid=(SENT // n,),
        in_specs=[rows, once(gate), once(up), once(down)],
        out_specs=rows,
        out_shape=jax.ShapeDtypeStruct((SENT, WIDTH), BF16),
        compiler_params=pltpu.CompilerParams(vmem_limit_bytes=48 << 20),
        cost_estimate=pl.CostEstimate(
            flops=20_000_000_000, bytes_accessed=24_000_000, transcendentals=1_600_000
        ),
    )(received, gate, up, down)


def exchange(x):
    return lax.all_to_all(x, SAME_CORE, split_axis=0, concat_axis=0, tiled=True)


def gather_kernel(back, high_ref, low_ref, mine_ref, theirs_ref):
    rows = back[...]
    both = nn(high_ref[...], rows) + nn(low_ref[...], rows)
    mine_ref[...] = both[0:ROWS]
    theirs_ref[...] = both[ROWS:]


def gathered(back, high, low):
    n = 256
    full = lambda *shape: pl.BlockSpec(shape, lambda s: (0,) * len(shape))
    part = pl.BlockSpec((ROWS, n), lambda s: (0, s))
    shape = jax.ShapeDtypeStruct((ROWS, WIDTH), F32)
    return pl.pallas_call(
        gather_kernel,
        name="gathered",
        grid=(WIDTH // n,),
        in_specs=[
            pl.BlockSpec((SENT, n), lambda s: (0, s)), full(2 * ROWS, SENT), full(2 * ROWS, SENT),
        ],
        out_specs=[part, part],
        out_shape=[shape, shape],
        compiler_params=pltpu.CompilerParams(vmem_limit_bytes=32 << 20),
        cost_estimate=pl.CostEstimate(
            flops=3_000_000_000, bytes_accessed=9_000_000, transcendentals=0
        ),
    )(back, high, low)


def from_other_core(a):
    return lax.ppermute(a, "ctx_2", [(0, 1), (1, 0)])


def local(
    residual, mixed_qkv, output_gate, log_decay, write_strength, conv_weight, norm_gain,
    out_weight, post_gain, router_weight, expert_ids, expert_gate, expert_up, expert_down,
    shared_gate, shared_up, shared_down, shared_switch,
):
    count = 128
    before = lax.ppermute(
        mixed_qkv[ROWS - 8 :], AXES, [(k, k + 1) for k in range(count - 1)]
    )
    half = WIDTH // 2
    own_half = lax.dynamic_slice_in_dim(out_weight, lax.axis_index("ctx_2") * half, half, 0)
    near = [
        lax.ppermute(own_half, "exp", [(k, (k + j) % 4) for k in range(4)]) for j in (1, 2, 3)
    ]
    far = [from_other_core(a) for a in near]
    maps, reads, offs = local_terms(mixed_qkv, before, conv_weight, log_decay, write_strength)
    starts = scan_states(maps)
    ids = jnp.concatenate([expert_ids, from_other_core(expert_ids)], axis=0)
    sel = slots(ids)
    after_mix, routed_in = mix(
        reads, offs, starts, output_gate, norm_gain.reshape(1, HEAD), residual,
        post_gain.reshape(1, WIDTH), out_weight, near, far,
    )
    outgoing, high, low = to_send(routed_in, from_other_core(routed_in), sel, ids, router_weight)
    received = exchange(outgoing.reshape(PEERS, SLOTS, WIDTH)).reshape(SENT, WIDTH)
    result = run_experts(received, expert_gate, expert_up, expert_down)
    returned = exchange(result.reshape(PEERS, SLOTS, WIDTH)).reshape(SENT, WIDTH)
    mine, theirs = gathered(returned, high, low)
    shared_hidden = (
        jax.nn.silu(jnp.dot(routed_in, shared_gate, preferred_element_type=F32))
        * jnp.dot(routed_in, shared_up, preferred_element_type=F32)
    ).astype(BF16)
    switch_rows = jax.nn.sigmoid(jnp.dot(routed_in, shared_switch, preferred_element_type=F32))
    shared_out = switch_rows[:, None] * jnp.dot(
        shared_hidden, shared_down, preferred_element_type=F32
    )
    return (after_mix.astype(F32) + shared_out + mine + from_other_core(theirs)).astype(BF16)


def solution(mesh):
    finer = Mesh(mesh.devices.reshape(4, 4, 2, mesh.shape["exp"]), AXES)
    rows = P(AXES, None)
    held = P(AXES, None, None)
    placed = (
        rows, rows, rows, rows, rows, P(), P(), P(None, "exp"), P(), P(), rows, held, held, held,
        P(), P(), P(), P(),
    )
    return jax.shard_map(local, mesh=finer, in_specs=placed, out_specs=rows, check_vma=False)
```

```python
import jax
import jax.numpy as jnp
import numpy as np
from jax import lax
from jax.experimental import pallas as pl
from jax.experimental.pallas import tpu as pltpu
from jax.sharding import Mesh
from jax.sharding import PartitionSpec as P

VHEADS = 16
HEAD = 128
ROWS = 128
TOP = 10
CAP = 6
WIDTH = 2048
EXPERTS = 256
AXES = ("ctx_0", "ctx_1", "ctx_2", "exp")
PEERS = 64
SLOTS = 4 * CAP
SENT = PEERS * SLOTS
BATCH = 8
MESH = pl.DeviceIdType.MESH
epsilon = 1e-06
F32 = jnp.float32
BF16 = jnp.bfloat16
VM = pl.BlockSpec(memory_space=pltpu.VMEM)
ANY = pl.BlockSpec(memory_space=pl.ANY)


def nn(a, b):
    return lax.dot_general(a, b, (((1,), (0,)), ((), ())), preferred_element_type=F32)


def nt(a, b):
    return lax.dot_general(a, b, (((1,), (1,)), ((), ())), preferred_element_type=F32)


def tn(a, b):
    return lax.dot_general(a, b, (((0,), (0,)), ((), ())), preferred_element_type=F32)


def silu(v):
    return v / (1.0 + jnp.exp(-v))


def local_kernel(
    q_ref, k_ref, v_ref, qb_ref, kb_ref, vb_ref, qw_ref, kw_ref, vw_ref, ld_ref, ws_ref,
    maps_ref, reads_ref, offs_ref, pad, cumt, lows, inv,
):
    first = pl.program_id(0) * BATCH
    rows = lax.broadcasted_iota(jnp.int32, (ROWS, ROWS), 0)
    cols = lax.broadcasted_iota(jnp.int32, (ROWS, ROWS), 1)
    causal = rows >= cols
    strict = rows > cols
    ones = causal.astype(F32)
    decay = ld_ref[...]
    highest = lax.Precision.HIGHEST
    cum = lax.dot_general(
        ones, decay, (((1,), (0,)), ((), ())), precision=highest, preferred_element_type=F32
    )
    cumt[...] = lax.dot_general(
        decay, ones, (((0,), (1,)), ((), ())), precision=highest, preferred_element_type=F32
    )
    strength = ws_ref[...]
    lane = lax.broadcasted_iota(jnp.int32, (ROWS, VHEADS), 1)

    def column(table, head):
        return jnp.sum(jnp.where(lane == head, table, 0.0), axis=1, keepdims=True)

    def activated(x_ref, b_ref, w_ref):
        n = x_ref.shape[1]
        pad[0:8, 0:n] = b_ref[...].astype(F32)
        pad[8 : 8 + ROWS, 0:n] = x_ref[...].astype(F32)
        total = w_ref[3:4, :] * pad[8 : 8 + ROWS, 0:n]
        for tap in range(3):
            total = total + w_ref[tap : tap + 1, :] * pad[5 + tap : 5 + tap + ROWS, 0:n]
        return silu(total)

    def unit(a):
        return a * lax.rsqrt(jnp.sum(a * a, axis=-1, keepdims=True) + epsilon)

    queries = activated(q_ref, qb_ref, qw_ref)
    keys = activated(k_ref, kb_ref, kw_ref)
    values = activated(v_ref, vb_ref, vw_ref)
    eye = (rows == cols).astype(F32)
    per_head = []
    for pair in range(BATCH // 2):
        part = slice(pair * HEAD, (pair + 1) * HEAD)
        query = unit(queries[:, part]) * HEAD ** (-0.5)
        key = unit(keys[:, part])
        key_b = key.astype(BF16)
        inner = nt(key_b, key_b)
        scores = nt(query.astype(BF16), key_b)
        for i in (2 * pair, 2 * pair + 1):
            c = column(cum, first + i)
            b = column(strength, first + i)
            gap = c - cumt[pl.ds(first + i, 1), :]
            ratios = jnp.where(causal, jnp.exp(jnp.where(causal, gap, 0.0)), 0.0)
            low = jnp.where(strict, ratios * inner, 0.0) * b
            lows[i] = low
            inv[i] = eye - jnp.where((rows >> 1) == (cols >> 1), low, 0.0)
            last = c[ROWS - 1 : ROWS, :]
            decays = jnp.exp(c)
            right = jnp.concatenate(
                [(b * decays * key).astype(BF16), (b * values[:, i * HEAD : (i + 1) * HEAD]).astype(BF16)],
                axis=1,
            )
            per_head.append(
                (
                    (scores * ratios).astype(BF16),
                    query * decays,
                    (key * jnp.exp(last - c)).astype(BF16),
                    right,
                    jnp.exp(last) - 1.0,
                )
            )
    for level in range(1, 7):
        here = ((rows >> (level + 1)) == (cols >> (level + 1))) & ((rows >> level) != (cols >> level))
        for i in range(BATCH):
            x = inv[i]
            x_b = x.astype(BF16)
            off = jnp.where(here, lows[i], 0.0).astype(BF16)
            inv[i] = x - nn(x_b, nn(off, x_b).astype(BF16))
    for i in range(BATCH):
        score, read, end_key, right, less = per_head[i]
        solved = nn(inv[i].astype(BF16), right).astype(BF16)
        carried = tn(solved, end_key)
        maps_ref[i, 0:HEAD, :] = (less * eye - carried[0:HEAD]).astype(BF16)
        maps_ref[i, HEAD : 2 * HEAD, :] = carried[HEAD:].astype(BF16)
        produced = nn(score, solved)
        reads_ref[i] = (read - produced[:, 0:HEAD]).astype(BF16)
        offs_ref[i] = produced[:, HEAD:]


def local_terms(mixed, before, conv_weight, log_decay, write_strength):
    n = BATCH // 2 * HEAD
    steps = VHEADS // BATCH

    def wide(rows_of, width, base):
        return pl.BlockSpec((rows_of, width), lambda s: (0, base + s))

    def three(rows_of):
        return [wide(rows_of, n, 0), wide(rows_of, n, steps), wide(rows_of, 2 * n, steps)]

    whole = pl.BlockSpec((ROWS, VHEADS), lambda s: (0, 0))
    return pl.pallas_call(
        local_kernel,
        name="local_terms",
        grid=(steps,),
        in_specs=three(ROWS) + three(8) + three(4) + [whole, whole],
        out_specs=[
            pl.BlockSpec((BATCH, 2 * HEAD, HEAD), lambda s: (s, 0, 0)),
            pl.BlockSpec((BATCH, ROWS, HEAD), lambda s: (s, 0, 0)),
            pl.BlockSpec((BATCH, ROWS, HEAD), lambda s: (s, 0, 0)),
        ],
        out_shape=[
            jax.ShapeDtypeStruct((VHEADS, 2 * HEAD, HEAD), BF16),
            jax.ShapeDtypeStruct((VHEADS, ROWS, HEAD), BF16),
            jax.ShapeDtypeStruct((VHEADS, ROWS, HEAD), F32),
        ],
        scratch_shapes=[
            pltpu.VMEM((8 + ROWS, 2 * n), F32),
            pltpu.VMEM((VHEADS, ROWS), F32),
            pltpu.VMEM((BATCH, ROWS, ROWS), F32),
            pltpu.VMEM((BATCH, ROWS, ROWS), F32),
        ],
        compiler_params=pltpu.CompilerParams(vmem_limit_bytes=40 << 20),
        cost_estimate=pl.CostEstimate(
            flops=8_000_000_000, bytes_accessed=6_000_000, transcendentals=1_000_000
        ),
    )(
        mixed, mixed, mixed, before, before, before, conv_weight, conv_weight, conv_weight,
        log_decay, write_strength,
    )


def scan_kernel(
    maps, weight, starts, wall, got1, pre1, tot1, got2, pre2, tot2, got3, st4, got4, st5, got5,
    send1, recv1, send2, recv2, send3, recv3, send4, recv4, send5, recv5,
    sendw1, recvw1, sendw2, recvw2, sendw3, recvw3,
):
    z, x, c, y = (lax.axis_index(a) for a in AXES)
    place = 2 * x + c
    barrier = pltpu.get_barrier_semaphore()

    def at(j, axis):
        if axis == "y":
            return {"exp": lax.rem(y + j, 4)}
        if axis == "z":
            return {"ctx_0": lax.rem(z + j, 4)}
        other = lax.rem(place + j, 8)
        return {"ctx_1": other // 2, "ctx_2": lax.rem(other, 2)}

    for axis, count in (("y", 4), ("z", 4), ("p", 8)):
        for j in range(1, count):
            pl.semaphore_signal(barrier, inc=1, device_id=at(j, axis), device_id_type=MESH)
    pl.semaphore_wait(barrier, 13)
    started = []

    def send(src, dst, s, r, device):
        copy = pltpu.make_async_remote_copy(
            src_ref=src, dst_ref=dst, send_sem=s, recv_sem=r, device_id=device, device_id_type=MESH
        )
        copy.start()
        started.append(copy)
        return copy

    copies = []
    for j in range(1, 4):
        other = lax.rem(y + j, 4)
        copies.append(
            send(maps.at[pl.ds(4 * other, 4)], got1.at[y], send1.at[j], recv1.at[j], at(j, "y"))
        )
    got1[y] = maps[pl.ds(4 * y, 4)]
    first = []
    for j in range(1, 4):
        for part, quarter in ((0, x), (1, z)):
            first.append(
                send(
                    weight.at[part, quarter, c], wall.at[y, part, quarter, c],
                    sendw1.at[j, part], recvw1.at[j, part], at(j, "y"),
                )
            )
    for copy in copies:
        copy.wait_recv()
    for h in range(4):
        run = got1[0, h].astype(F32)
        for m in range(1, 4):
            pre1[m - 1, h] = run.astype(BF16)
            run = run + got1[m, h].astype(F32) + nn(run.astype(BF16), got1[m, h, 0:HEAD, :])
        tot1[h] = run.astype(BF16)

    copies = []
    for j in range(1, 8):
        other = lax.rem(place + j, 8)
        head, half = other // 2, lax.rem(other, 2)
        copies.append(
            send(
                tot1.at[head, 0:HEAD], got2.at[place, 0:HEAD], send2.at[j, 0], recv2.at[j, 0],
                at(j, "p"),
            )
        )
        copies.append(
            send(
                tot1.at[head, pl.ds(pl.multiple_of(HEAD + 64 * half, 64), 64)],
                got2.at[place, HEAD : HEAD + 64],
                send2.at[j, 1], recv2.at[j, 1], at(j, "p"),
            )
        )
    got2[place, 0:HEAD, :] = tot1[x, 0:HEAD, :]
    got2[place, HEAD : HEAD + 64, :] = tot1[x, pl.ds(pl.multiple_of(HEAD + 64 * c, 64), 64), :]
    for copy in copies:
        copy.wait_recv()
    run = got2[0].astype(F32)
    for p in range(1, 8):
        pre2[p - 1] = run.astype(BF16)
        run = run + got2[p].astype(F32) + nn(run.astype(BF16), got2[p, 0:HEAD, :])
    tot2[...] = run.astype(BF16)

    copies = []
    for j in range(1, 4):
        copies.append(send(tot2, got3.at[z], send3.at[j], recv3.at[j], at(j, "z")))
    got3[z] = tot2[...]
    for copy in copies:
        copy.wait_recv()
    state = jnp.zeros((64, HEAD), F32)
    for k in range(3):
        later = state + got3[k, HEAD:, :].astype(F32) + nn(state.astype(BF16), got3[k, 0:HEAD, :])
        state = jnp.where(k < z, later, state)
    state_b = state.astype(BF16)
    st4[0] = state_b
    for p in range(1, 8):
        st4[p] = (
            state + pre2[p - 1, HEAD:, :].astype(F32) + nn(state_b, pre2[p - 1, 0:HEAD, :])
        ).astype(BF16)

    copies = []
    rows_here = pl.ds(pl.multiple_of(64 * c, 64), 64)
    for j in range(1, 8):
        other = lax.rem(place + j, 8)
        copies.append(
            send(st4.at[other], got4.at[x, rows_here], send4.at[j], recv4.at[j], at(j, "p"))
        )
    got4[x, rows_here, :] = st4[place]
    for copy in first:
        copy.wait_recv()
    second = []
    for k in range(1, 4):
        for j in range(1, 4):
            other = lax.rem(y + j, 4)
            for part, quarter, device in (
                (0, x, {"ctx_1": lax.rem(x + k, 4)}),
                (1, z, {"ctx_0": lax.rem(z + k, 4)}),
            ):
                held = wall.at[other, part, quarter, c]
                second.append(
                    send(held, held, sendw2.at[k, j, part], recvw2.at[k, j, part], device)
                )
    for copy in copies:
        copy.wait_recv()
    for h in range(4):
        begin = got4[h]
        st5[0, h] = begin
        for m in range(1, 4):
            st5[m, h] = (
                begin.astype(F32)
                + pre1[m - 1, h, HEAD:, :].astype(F32)
                + nn(begin, pre1[m - 1, h, 0:HEAD, :])
            ).astype(BF16)

    copies = []
    for j in range(1, 4):
        other = lax.rem(y + j, 4)
        copies.append(send(st5.at[other], got5.at[y], send5.at[j], recv5.at[j], at(j, "y")))
    got5[y] = st5[y]
    for copy in copies:
        copy.wait_recv()
    for m in range(4):
        starts[4 * m : 4 * m + 4] = got5[m]
    for copy in second:
        copy.wait_recv()
    third = []
    for j in range(1, 4):
        held = wall.at[lax.rem(y + j, 4), :, :, c]
        third.append(send(held, held, sendw3.at[j], recvw3.at[j], {"ctx_2": 1 - c}))
    for copy in third:
        copy.wait_recv()
    for copy in started:
        copy.wait_send()


def scan_states(maps, out_weight):
    dma = pltpu.SemaphoreType.DMA
    cut = (2, 4, 2, WIDTH // 16, WIDTH // 4)
    return pl.pallas_call(
        scan_kernel,
        name="scan_states",
        in_specs=[VM, ANY],
        out_specs=[VM, ANY],
        out_shape=[
            jax.ShapeDtypeStruct((VHEADS, HEAD, HEAD), BF16),
            jax.ShapeDtypeStruct((4, *cut), BF16),
        ],
        scratch_shapes=[
            pltpu.VMEM((4, 4, 2 * HEAD, HEAD), BF16),
            pltpu.VMEM((3, 4, 2 * HEAD, HEAD), BF16),
            pltpu.VMEM((4, 2 * HEAD, HEAD), BF16),
            pltpu.VMEM((8, HEAD + 64, HEAD), BF16),
            pltpu.VMEM((7, HEAD + 64, HEAD), BF16),
            pltpu.VMEM((HEAD + 64, HEAD), BF16),
            pltpu.VMEM((4, HEAD + 64, HEAD), BF16),
            pltpu.VMEM((8, 64, HEAD), BF16),
            pltpu.VMEM((4, HEAD, HEAD), BF16),
            pltpu.VMEM((4, 4, HEAD, HEAD), BF16),
            pltpu.VMEM((4, 4, HEAD, HEAD), BF16),
            dma((4,)), dma((4,)), dma((8, 2)), dma((8, 2)), dma((4,)), dma((4,)),
            dma((8,)), dma((8,)), dma((4,)), dma((4,)),
            dma((4, 2)), dma((4, 2)), dma((4, 4, 2)), dma((4, 4, 2)), dma((4,)), dma((4,)),
        ],
        compiler_params=pltpu.CompilerParams(
            collective_id=0, has_side_effects=True, vmem_limit_bytes=32 << 20
        ),
        cost_estimate=pl.CostEstimate(
            flops=30_000_000_000, bytes_accessed=4_000_000, transcendentals=0
        ),
    )(maps, out_weight.reshape(cut))


def mix_kernel(
    reads, offs, starts, gate_ref, gain_ref, res_ref, post_ref, own, wall,
    after_ref, routed_ref, weights, normed, total, sems,
):
    y = lax.axis_index("exp")
    loads = [[pltpu.make_async_copy(own, weights.at[0], sems.at[0])]]
    for j in range(1, 4):
        loads.append(
            [pltpu.make_async_copy(wall.at[lax.rem(y + j, 4)], weights.at[j], sems.at[j])]
        )
    for group in loads:
        for load in group:
            load.start()
    gain = gain_ref[...]
    for h in range(VHEADS):
        part = slice(h * HEAD, (h + 1) * HEAD)
        out = offs[h] + nt(reads[h], starts[h])
        out = out * lax.rsqrt(jnp.mean(out * out, axis=-1, keepdims=True) + epsilon)
        normed[:, part] = (out * gain * silu(gate_ref[:, part].astype(F32))).astype(BF16)
    columns = WIDTH // 4
    for j in range(4):
        for load in loads[j]:
            load.wait()
        block = lax.rem(y + j, 4)
        here = pl.ds(pl.multiple_of(columns * block, columns), columns)
        total[:, here] = nn(normed[...], weights[j])
    after = (res_ref[...].astype(F32) + total[...]).astype(BF16)
    after_ref[...] = after
    wide = after.astype(F32)
    routed_ref[...] = (
        wide * lax.rsqrt(jnp.mean(wide * wide, axis=-1, keepdims=True) + epsilon) * post_ref[...]
    ).astype(BF16)


def mix(reads, offs, starts, gate, gain, residual, post, own, wall):
    shape = jax.ShapeDtypeStruct((ROWS, WIDTH), BF16)
    return pl.pallas_call(
        mix_kernel,
        name="mix",
        in_specs=[VM] * 7 + [ANY] * 2,
        out_specs=[VM, VM],
        out_shape=[shape, shape],
        scratch_shapes=[
            pltpu.VMEM((4, WIDTH, WIDTH // 4), BF16),
            pltpu.VMEM((ROWS, WIDTH), BF16),
            pltpu.VMEM((ROWS, WIDTH), F32),
            pltpu.SemaphoreType.DMA((4,)),
        ],
        compiler_params=pltpu.CompilerParams(vmem_limit_bytes=40 << 20),
        cost_estimate=pl.CostEstimate(
            flops=2_000_000_000, bytes_accessed=12_000_000, transcendentals=300_000
        ),
    )(reads, offs, starts, gate, gain, residual, post, own, wall.reshape(4, WIDTH, WIDTH // 4))


def distance(group, i):
    dx = lax.rem(i, 4)
    dy = lax.rem(dx + lax.rem(group, 4), 4)
    dz = lax.rem(dx + 2 * (i // 4) + group // 4, 4)
    return dz, dx, dy


LANES = np.arange(SENT)
PEER, INSIDE = LANES // SLOTS, LANES % SLOTS
NEAR = PEER % 8
TABLE = np.stack(
    [
        (NEAR + 2 * (NEAR // 4) + PEER // 32) % 4,
        NEAR % 4,
        (NEAR + PEER // 8) % 4,
        INSIDE // (2 * CAP),
        INSIDE % (2 * CAP) // CAP,
        INSIDE % CAP,
        0 * LANES,
        0 * LANES,
    ]
).astype(np.int32)


def wanted_experts(table_ref, lanes=slice(None)):
    z, x, c, y = (lax.axis_index(a) for a in AXES)
    there = ((table_ref[0:1, lanes] + z) & 3) * 32 + ((table_ref[1:2, lanes] + x) & 3) * 8
    there = there + c * 4 + ((table_ref[2:3, lanes] + y) & 3)
    return 2 * there + table_ref[3:4, lanes]


def slot_kernel(ids_ref, table_ref, sel_ref):
    wanted = wanted_experts(table_ref)
    source, slot = table_ref[4:5, :], table_ref[5:6, :]
    rows = lax.broadcasted_iota(jnp.int32, (ROWS, ROWS), 0)
    cols = lax.broadcasted_iota(jnp.int32, (ROWS, ROWS), 1)
    earlier = (rows > cols).astype(BF16)
    for half in range(2):
        part = slice(half * ROWS, (half + 1) * ROWS)
        ids = ids_ref[part, :]
        aim = jnp.where(source == half, wanted, -1)
        hit = ids[:, 0:1] == aim
        for k in range(1, TOP):
            hit = hit | (ids[:, k : k + 1] == aim)
        marks = hit.astype(F32)
        rank = nn(earlier, marks.astype(BF16))
        sel_ref[part, :] = jnp.where(rank == slot.astype(F32), marks, 0.0).astype(BF16)


def slots(ids):
    return pl.pallas_call(
        slot_kernel,
        name="slots",
        in_specs=[VM, VM],
        out_specs=VM,
        out_shape=jax.ShapeDtypeStruct((2 * ROWS, SENT), BF16),
        compiler_params=pltpu.CompilerParams(vmem_limit_bytes=32 << 20),
        cost_estimate=pl.CostEstimate(
            flops=200_000_000, bytes_accessed=1_000_000, transcendentals=0
        ),
    )(ids, jnp.asarray(TABLE))


GROUPS, EACH = 8, 8
BUILT = 2 * EACH * SLOTS


def moe_kernel(
    routed, after, sel, ids_ref, table_ref, switch, router, s_gate, s_up, s_down, gate, up, down,
    out_ref, rows2, out_buf, in_buf, back_buf, high, low, total, swap, theirs,
    v_router, v_sgate, v_sup, v_sdown, v_gate, v_up, v_down,
    load_sems, send_x, recv_x, send1, recv1, send2, recv2, send_y, recv_y,
):
    z, x, c, y = (lax.axis_index(a) for a in AXES)
    partner = {"ctx_2": 1 - c}
    barrier = pltpu.get_barrier_semaphore()

    def peer(group, i, sign):
        dz, dx, dy = distance(group, i)
        return {
            "ctx_0": lax.rem(z + 4 + sign * dz, 4),
            "ctx_1": lax.rem(x + 4 + sign * dx, 4),
            "exp": lax.rem(y + 4 + sign * dy, 4),
        }

    def greet(k, _):
        pl.semaphore_signal(
            barrier, inc=1, device_id=peer(k // EACH, lax.rem(k, EACH), 1), device_id_type=MESH
        )
        return 0

    lax.fori_loop(1, PEERS, greet, 0)
    pl.semaphore_signal(barrier, inc=1, device_id=partner, device_id_type=MESH)
    loads = [
        pltpu.make_async_copy(src, dst, load_sems.at[k])
        for k, (src, dst) in enumerate(
            (
                (router, v_router), (s_gate, v_sgate), (s_up, v_sup), (s_down, v_sdown),
                (gate, v_gate), (up, v_up), (down, v_down),
            )
        )
    ]
    for load in loads:
        load.start()
    pl.semaphore_wait(barrier, PEERS)

    both = pltpu.make_async_remote_copy(
        src_ref=routed, dst_ref=rows2.at[ROWS : 2 * ROWS], send_sem=send_x, recv_sem=recv_x,
        device_id=partner, device_id_type=MESH,
    )
    both.start()
    rows2[0:ROWS, :] = routed[...]
    both.wait_recv()

    def remote(src, dst, s, r, device):
        return pltpu.make_async_remote_copy(
            src_ref=src, dst_ref=dst, send_sem=s, recv_sem=r, device_id=device, device_id_type=MESH
        )

    def dispatch(group, begin):
        def one(i, _):
            g = group * EACH + i
            remote(
                out_buf.at[g], in_buf.at[g], send1.at[group], recv1.at[group], peer(group, i, 1)
            ).start()
            return 0

        lax.fori_loop(begin, EACH, one, 0)

    def give_back(group, begin):
        def one(i, _):
            g = group * EACH + i
            remote(
                in_buf.at[g], back_buf.at[g], send2.at[group], recv2.at[group], peer(group, i, -1)
            ).start()
            return 0

        lax.fori_loop(begin, EACH, one, 0)

    for p in range(GROUPS // 2):
        lanes = slice(p * BUILT, (p + 1) * BUILT)
        built = tn(sel[:, lanes], rows2[...]).astype(BF16)
        out_buf[2 * p * EACH : 2 * (p + 1) * EACH] = built.reshape(2 * EACH, SLOTS, WIDTH)
        dispatch(2 * p, 0 if p else 1)
        dispatch(2 * p + 1, 0)
        if p == 0:
            pltpu.make_async_copy(out_buf.at[0], in_buf.at[0], recv1.at[0]).start()

    loads[0].wait()
    logits = nn(rows2[...], v_router[...])
    lane = lax.broadcasted_iota(jnp.int32, (2 * ROWS, EXPERTS), 1)
    ids = ids_ref[...]
    hit = ids[:, 0:1] == lane
    for k in range(1, TOP):
        hit = hit | (ids[:, k : k + 1] == lane)
    chosen = jnp.where(hit, jnp.exp(jnp.where(hit, logits, 0.0)), 0.0)
    gates = chosen / jnp.sum(chosen, axis=1, keepdims=True)
    gates_high = gates.astype(BF16)
    gates_low = (gates - gates_high.astype(F32)).astype(BF16)
    for p in range(GROUPS // 2):
        lanes = slice(p * BUILT, (p + 1) * BUILT)
        spread = (
            lax.broadcasted_iota(jnp.int32, (EXPERTS, BUILT), 0) == wanted_experts(table_ref, lanes)
        ).astype(BF16)
        high[p] = nn(gates_high, spread).astype(BF16) * sel[:, lanes]
        low[p] = nn(gates_low, spread).astype(BF16) * sel[:, lanes]

    for load in loads[1:4]:
        load.wait()
    mine = routed[...]
    hidden = (silu(nn(mine, v_sgate[...])) * nn(mine, v_sup[...])).astype(BF16)
    open_ = jnp.sum(mine.astype(F32) * switch[...].astype(F32), axis=1, keepdims=True)
    total[0:ROWS, :] = after[...].astype(F32) + nn(hidden, v_sdown[...]) / (1.0 + jnp.exp(-open_))
    total[ROWS:, :] = jnp.zeros((ROWS, WIDTH), F32)

    for load in loads[4:]:
        load.wait()

    def serve(group, begin):
        here = pl.ds(group * EACH, EACH)
        pltpu.make_async_copy(in_buf.at[here], in_buf.at[here], recv1.at[group]).wait()
        n = EACH * SLOTS
        rows = in_buf[here].reshape(n, WIDTH)
        inside = lax.rem(lax.broadcasted_iota(jnp.int32, (n, 1), 0), SLOTS)
        result = None
        for e in range(2):
            hidden = silu(nn(rows, v_gate[e])) * nn(rows, v_up[e])
            hidden = jnp.where((inside >= 2 * CAP) == bool(e), hidden, 0.0).astype(BF16)
            part = nn(hidden, v_down[e])
            result = part if result is None else result + part
        in_buf[here] = result.astype(BF16).reshape(EACH, SLOTS, WIDTH)

    serve(0, 1)
    pltpu.make_async_copy(in_buf.at[0], back_buf.at[0], recv2.at[0]).start()
    give_back(0, 1)

    def later(group, _):
        serve(group, 0)
        give_back(group, 0)
        return 0

    lax.fori_loop(1, GROUPS, later, 0)

    for p in range(GROUPS // 2):
        for group in (2 * p, 2 * p + 1):
            here = pl.ds(group * EACH, EACH)
            pltpu.make_async_copy(back_buf.at[here], back_buf.at[here], recv2.at[group]).wait()
        rows = back_buf[2 * p * EACH : 2 * (p + 1) * EACH].reshape(BUILT, WIDTH)
        total[...] += nn(high[p], rows) + nn(low[p], rows)

    theirs[...] = total[ROWS:, :]
    last = remote(theirs, swap, send_y, recv_y, partner)
    last.start()
    last.wait_recv()
    out_ref[...] = (total[0:ROWS, :] + swap[...]).astype(BF16)

    both.wait_send()
    last.wait_send()
    for group in range(GROUPS):
        here = pl.ds(1, EACH - 1) if group == 0 else pl.ds(group * EACH, EACH)
        pltpu.make_async_copy(out_buf.at[here], out_buf.at[here], send1.at[group]).wait()
        pltpu.make_async_copy(in_buf.at[here], in_buf.at[here], send2.at[group]).wait()


def experts(
    routed, after, sel, ids, switch, router, s_gate, s_up, s_down, gate, up, down
):
    dma = pltpu.SemaphoreType.DMA
    vmem = lambda a: pltpu.VMEM(a.shape, a.dtype)
    slabs = pltpu.VMEM((PEERS, SLOTS, WIDTH), BF16)
    weights = (router, s_gate, s_up, s_down, gate, up, down)
    return pl.pallas_call(
        moe_kernel,
        name="experts",
        in_specs=[VM] * 6 + [ANY] * 7,
        out_specs=VM,
        out_shape=jax.ShapeDtypeStruct((ROWS, WIDTH), BF16),
        scratch_shapes=[
            pltpu.VMEM((2 * ROWS, WIDTH), BF16),
            slabs, slabs, slabs,
            pltpu.VMEM((GROUPS // 2, 2 * ROWS, BUILT), BF16),
            pltpu.VMEM((GROUPS // 2, 2 * ROWS, BUILT), BF16),
            pltpu.VMEM((2 * ROWS, WIDTH), F32),
            pltpu.VMEM((ROWS, WIDTH), F32),
            pltpu.VMEM((ROWS, WIDTH), F32),
            *(vmem(w) for w in weights),
            dma((7,)), dma, dma, dma((GROUPS,)), dma((GROUPS,)), dma((GROUPS,)), dma((GROUPS,)),
            dma, dma,
        ],
        compiler_params=pltpu.CompilerParams(
            collective_id=1, has_side_effects=True, vmem_limit_bytes=62 << 20
        ),
        cost_estimate=pl.CostEstimate(
            flops=60_000_000_000, bytes_accessed=30_000_000, transcendentals=2_000_000
        ),
    )(routed, after, sel, ids, jnp.asarray(TABLE), switch, *weights)


def from_other_core(a):
    return lax.ppermute(a, "ctx_2", [(0, 1), (1, 0)])


def local(
    residual, mixed_qkv, output_gate, log_decay, write_strength, conv_weight, norm_gain,
    out_weight, post_gain, router_weight, expert_ids, expert_gate, expert_up, expert_down,
    shared_gate, shared_up, shared_down, shared_switch,
):
    count = 128
    before = lax.ppermute(
        mixed_qkv[ROWS - 8 :], AXES, [(k, k + 1) for k in range(count - 1)]
    )
    ids = jnp.concatenate([expert_ids, from_other_core(expert_ids)], axis=0)
    sel = slots(ids)
    before, sel = lax.optimization_barrier((before, sel))
    maps, reads, offs = local_terms(mixed_qkv, before, conv_weight, log_decay, write_strength)
    starts, wall = scan_states(maps, out_weight)
    after_mix, routed_in = mix(
        reads, offs, starts, output_gate, norm_gain.reshape(1, HEAD), residual,
        post_gain.reshape(1, WIDTH), out_weight, wall,
    )
    return experts(
        routed_in, after_mix, sel, ids, shared_switch.reshape(1, WIDTH), router_weight,
        shared_gate, shared_up, shared_down, expert_gate, expert_up, expert_down,
    )


def solution(mesh):
    finer = Mesh(mesh.devices.reshape(4, 4, 2, mesh.shape["exp"]), AXES)
    rows = P(AXES, None)
    held = P(AXES, None, None)
    placed = (
        rows, rows, rows, rows, rows, P(), P(), P(None, "exp"), P(), P(), rows, held, held, held,
        P(), P(), P(), P(),
    )
    return jax.shard_map(local, mesh=finer, in_specs=placed, out_specs=rows, check_vma=False)
```

```python
import jax
import jax.numpy as jnp
import numpy as np
from jax import lax
from jax.experimental import pallas as pl
from jax.experimental.pallas import tpu as pltpu
from jax.sharding import Mesh
from jax.sharding import PartitionSpec as P

VHEADS = 16
HEAD = 128
ROWS = 128
TOP = 10
CAP = 6
WIDTH = 2048
EXPERTS = 256
AXES = ("ctx_0", "ctx_1", "ctx_2", "exp")
PEERS = 64
SLOTS = 4 * CAP
SENT = PEERS * SLOTS
BATCH = 8
MESH = pl.DeviceIdType.MESH
epsilon = 1e-06
F32 = jnp.float32
BF16 = jnp.bfloat16
VM = pl.BlockSpec(memory_space=pltpu.VMEM)
ANY = pl.BlockSpec(memory_space=pl.ANY)


def nn(a, b):
    return lax.dot_general(a, b, (((1,), (0,)), ((), ())), preferred_element_type=F32)


def nt(a, b):
    return lax.dot_general(a, b, (((1,), (1,)), ((), ())), preferred_element_type=F32)


def tn(a, b):
    return lax.dot_general(a, b, (((0,), (0,)), ((), ())), preferred_element_type=F32)


def silu(v):
    return v / (1.0 + jnp.exp(-v))


def front_kernel(
    mixed, conv, decay_ref, strength_ref, ids_ref, table_ref, gate_ref, gain_ref, res_ref,
    post_ref, weight,
    after_ref, routed_ref, sel_ref, all_ids,
    there, tail, ids_there, pad, cumt, lows, inv, maps, reads, offs, wall, normed, mixed_rows,
    got1, pre1, tot1, got2, pre2, tot2, got3, st4, got4, st5, got5,
    own_sem, send0, recv0, send1, recv1, send2, recv2, send3, recv3, send4, recv4, send5, recv5,
    sendw1, recvw1, sendw2, recvw2, sendw3, recvw3,
):
    z, x, c, y = (lax.axis_index(a) for a in AXES)
    place = 2 * x + c
    spot = (z * 4 + x) * 8 + c * 4 + y
    partner = {"ctx_2": 1 - c}
    barrier = pltpu.get_barrier_semaphore()

    def whole(k):
        return {
            "ctx_0": k // 32, "ctx_1": lax.rem(k // 8, 4), "ctx_2": lax.rem(k // 4, 2),
            "exp": lax.rem(k, 4),
        }

    following, previous = whole(lax.rem(spot + 1, 128)), whole(lax.rem(spot + 127, 128))

    def at(j, axis):
        if axis == "y":
            return {"exp": lax.rem(y + j, 4)}
        if axis == "z":
            return {"ctx_0": lax.rem(z + j, 4)}
        if axis == "x":
            return {"ctx_1": lax.rem(x + j, 4)}
        other = lax.rem(place + j, 8)
        return {"ctx_1": other // 2, "ctx_2": lax.rem(other, 2)}

    for device in (following, previous):
        pl.semaphore_signal(barrier, inc=1, device_id=device, device_id_type=MESH)
    for axis, count in (("y", 4), ("z", 4), ("p", 8)):
        for j in range(1, count):
            pl.semaphore_signal(barrier, inc=1, device_id=at(j, axis), device_id_type=MESH)
    own = pltpu.make_async_copy(weight, wall.at[y], own_sem)
    own.start()
    pl.semaphore_wait(barrier, 15)
    started = []

    def remote(src, dst, s, r, device):
        return pltpu.make_async_remote_copy(
            src_ref=src, dst_ref=dst, send_sem=s, recv_sem=r, device_id=device, device_id_type=MESH
        )

    def send(*args):
        copy = remote(*args)
        copy.start()
        started.append(copy)
        return copy

    last_rows = send(mixed.at[ROWS - 16 : ROWS], tail, send0.at[0], recv0.at[0], following)
    ids_copy = send(ids_ref, ids_there, send0.at[1], recv0.at[1], partner)
    first = []
    for j in range(1, 4):
        for part, quarter in ((0, x), (1, z)):
            first.append(
                send(
                    weight.at[part, quarter, c], wall.at[y, part, quarter, c],
                    sendw1.at[j, part], recvw1.at[j, part], at(j, "y"),
                )
            )

    rows = lax.broadcasted_iota(jnp.int32, (ROWS, ROWS), 0)
    cols = lax.broadcasted_iota(jnp.int32, (ROWS, ROWS), 1)
    causal = rows >= cols
    strict = rows > cols
    ones = causal.astype(F32)
    eye = (rows == cols).astype(F32)
    eye_b = eye.astype(BF16)

    earlier = strict.astype(BF16)
    wanted = wanted_experts(table_ref)
    source, slot = table_ref[4:5, :], table_ref[5:6, :]
    ids_copy.wait_recv()
    for half, held in ((0, ids_ref), (1, ids_there)):
        ids = nt(eye_b, held[...].astype(F32).astype(BF16))
        all_ids[half * ROWS : (half + 1) * ROWS, :] = ids
        aim = jnp.where(source == half, wanted, -1).astype(F32)
        hit = ids[:, 0:1] == aim
        for k in range(1, TOP):
            hit = hit | (ids[:, k : k + 1] == aim)
        marks = hit.astype(F32)
        rank = nn(earlier, marks.astype(BF16))
        sel_ref[half * ROWS : (half + 1) * ROWS, :] = jnp.where(
            rank == slot.astype(F32), marks, 0.0
        ).astype(BF16)

    decay, highest = decay_ref[...], lax.Precision.HIGHEST

    def exact(p, q):
        return lax.dot_general(
            p, q, (((1,), (1,)), ((), ())), precision=highest, preferred_element_type=F32
        )

    cum = exact(ones, decay)
    cumt[...] = exact(decay, ones)
    strength = exact(eye, strength_ref[...])
    lane = lax.broadcasted_iota(jnp.int32, (ROWS, VHEADS), 1)

    def column(table, head):
        return jnp.sum(jnp.where(lane == head, table, 0.0), axis=1, keepdims=True)

    def activated(begin, n):
        here = pl.ds(pl.multiple_of(begin, HEAD), n)
        pad[0:8, 0:n] = jnp.where(spot > 0, tail[8:16, here].astype(F32), 0.0)
        pad[8 : 8 + ROWS, 0:n] = mixed[:, here].astype(F32)
        total = conv[3:4, here] * pad[8 : 8 + ROWS, 0:n]
        for tap in range(3):
            total = total + conv[tap : tap + 1, here] * pad[5 + tap : 5 + tap + ROWS, 0:n]
        return silu(total)

    def unit(a):
        return a * lax.rsqrt(jnp.sum(a * a, axis=-1, keepdims=True) + epsilon)

    last_rows.wait_recv()

    def terms(batch, _):
        groups = [lax.rem(y + 1 + 2 * batch + part, 4) for part in range(2)]
        heads = [4 * groups[i // 4] + i % 4 for i in range(BATCH)]
        n = 2 * HEAD
        queries = [activated(g * n, n) for g in groups]
        keys = [activated(WIDTH // 2 + g * n, n) for g in groups]
        values = [activated(WIDTH + 2 * g * n, 2 * n) for g in groups]
        per_head = []
        for pair in range(BATCH // 2):
            part = slice(pair % 2 * HEAD, (pair % 2 + 1) * HEAD)
            query = unit(queries[pair // 2][:, part]) * HEAD ** (-0.5)
            key = unit(keys[pair // 2][:, part])
            key_b = key.astype(BF16)
            inner = nt(key_b, key_b)
            scores = nt(query.astype(BF16), key_b)
            for i in (2 * pair, 2 * pair + 1):
                d = column(cum, heads[i])
                b = column(strength, heads[i])
                gap = d - cumt[pl.ds(heads[i], 1), :]
                ratios = jnp.where(causal, jnp.exp(jnp.where(causal, gap, 0.0)), 0.0)
                low = jnp.where(strict, ratios * inner, 0.0) * b
                lows[i] = low
                inv[i] = eye - jnp.where((rows >> 1) == (cols >> 1), low, 0.0)
                end = d[ROWS - 1 : ROWS, :]
                decays = jnp.exp(d)
                right = jnp.concatenate(
                    [
                        (b * decays * key).astype(BF16),
                        (b * values[i // 4][:, i % 4 * HEAD : (i % 4 + 1) * HEAD]).astype(BF16),
                    ],
                    axis=1,
                )
                per_head.append(
                    (
                        (scores * ratios).astype(BF16),
                        query * decays,
                        (key * jnp.exp(end - d)).astype(BF16),
                        right,
                        jnp.exp(end) - 1.0,
                    )
                )
        for level in range(1, 7):
            here = (rows >> (level + 1)) == (cols >> (level + 1))
            here = here & ((rows >> level) != (cols >> level))
            for i in range(BATCH):
                now = inv[i]
                now_b = now.astype(BF16)
                off = jnp.where(here, lows[i], 0.0).astype(BF16)
                inv[i] = now - nn(now_b, nn(off, now_b).astype(BF16))
        for i in range(BATCH):
            score, read, end_key, right, less = per_head[i]
            solved = nn(inv[i].astype(BF16), right).astype(BF16)
            carried = tn(solved, end_key)
            maps[heads[i], 0:HEAD, :] = (less * eye - carried[0:HEAD]).astype(BF16)
            maps[heads[i], HEAD : 2 * HEAD, :] = carried[HEAD:].astype(BF16)
            produced = nn(score, solved)
            reads[heads[i]] = (read - produced[:, 0:HEAD]).astype(BF16)
            offs[heads[i]] = produced[:, HEAD:]
        for other in groups:
            four = maps.at[pl.ds(4 * other, 4)]

            @pl.when(other != y)
            def _():
                remote(four, got1.at[y], send1.at[other], recv1.at[y], {"exp": other}).start()

            @pl.when(other == y)
            def _():
                pltpu.make_async_copy(four, got1.at[y], recv1.at[y]).start()

        return 0

    lax.fori_loop(0, VHEADS // BATCH, terms, 0)

    for copy in first:
        copy.wait_recv()

    def spread(k):
        copies = []
        for j in range(1, 4):
            other = lax.rem(y + j, 4)
            for part, quarter, device in ((0, x, at(k, "x")), (1, z, at(k, "z"))):
                held = wall.at[other, part, quarter, c]
                copies.append(
                    send(held, held, sendw2.at[k, j, part], recvw2.at[k, j, part], device)
                )
        return copies

    def across(k):
        copies = []
        for j in range(1, 4):
            other = lax.rem(y + j, 4)
            for part, quarter in ((0, lax.rem(x + 4 - k, 4)), (1, lax.rem(z + 4 - k, 4))):
                held = wall.at[other, part, quarter, c]
                copies.append(
                    send(held, held, sendw3.at[k, j, part], recvw3.at[k, j, part], partner)
                )
        return copies

    second = spread(1) + spread(3)
    third = across(0)

    for m in range(4):
        pltpu.make_async_copy(got1.at[m], got1.at[m], recv1.at[m]).wait()
    for h in range(4):
        run = got1[0, h].astype(F32)
        for m in range(1, 4):
            pre1[m - 1, h] = run.astype(BF16)
            run = run + got1[m, h].astype(F32) + nn(run.astype(BF16), got1[m, h, 0:HEAD, :])
        tot1[h] = run.astype(BF16)

    copies = []
    for j in range(1, 8):
        other = lax.rem(place + j, 8)
        head, half = other // 2, lax.rem(other, 2)
        copies.append(
            send(
                tot1.at[head, 0:HEAD], got2.at[place, 0:HEAD], send2.at[j, 0], recv2.at[j, 0],
                at(j, "p"),
            )
        )
        copies.append(
            send(
                tot1.at[head, pl.ds(pl.multiple_of(HEAD + 64 * half, 64), 64)],
                got2.at[place, HEAD : HEAD + 64],
                send2.at[j, 1], recv2.at[j, 1], at(j, "p"),
            )
        )
    got2[place, 0:HEAD, :] = tot1[x, 0:HEAD, :]
    got2[place, HEAD : HEAD + 64, :] = tot1[x, pl.ds(pl.multiple_of(HEAD + 64 * c, 64), 64), :]
    for copy in copies:
        copy.wait_recv()
    run = got2[0].astype(F32)
    for p in range(1, 8):
        pre2[p - 1] = run.astype(BF16)
        run = run + got2[p].astype(F32) + nn(run.astype(BF16), got2[p, 0:HEAD, :])
    tot2[...] = run.astype(BF16)

    copies = []
    for j in range(1, 4):
        copies.append(send(tot2, got3.at[z], send3.at[j], recv3.at[j], at(j, "z")))
    got3[z] = tot2[...]
    for copy in copies:
        copy.wait_recv()
    state = jnp.zeros((64, HEAD), F32)
    for k in range(3):
        later = state + got3[k, HEAD:, :].astype(F32) + nn(state.astype(BF16), got3[k, 0:HEAD, :])
        state = jnp.where(k < z, later, state)
    state_b = state.astype(BF16)
    st4[0] = state_b
    for p in range(1, 8):
        st4[p] = (
            state + pre2[p - 1, HEAD:, :].astype(F32) + nn(state_b, pre2[p - 1, 0:HEAD, :])
        ).astype(BF16)

    copies = []
    rows_here = pl.ds(pl.multiple_of(64 * c, 64), 64)
    for j in range(1, 8):
        other = lax.rem(place + j, 8)
        copies.append(
            send(st4.at[other], got4.at[x, rows_here], send4.at[j], recv4.at[j], at(j, "p"))
        )
    got4[x, rows_here, :] = st4[place]
    second_last = spread(2)
    for copy in second:
        copy.wait_recv()
    third += across(1) + across(3)
    for copy in copies:
        copy.wait_recv()
    for h in range(4):
        begin = got4[h]
        st5[0, h] = begin
        for m in range(1, 4):
            st5[m, h] = (
                begin.astype(F32)
                + pre1[m - 1, h, HEAD:, :].astype(F32)
                + nn(begin, pre1[m - 1, h, 0:HEAD, :])
            ).astype(BF16)

    copies = []
    for j in range(1, 4):
        other = lax.rem(y + j, 4)
        copies.append(send(st5.at[other], got5.at[y], send5.at[j], recv5.at[j], at(j, "y")))
    got5[y] = st5[y]
    for copy in second_last:
        copy.wait_recv()
    third += across(2)
    for copy in copies:
        copy.wait_recv()

    gain = gain_ref[...]
    for h in range(VHEADS):
        part = slice(h * HEAD, (h + 1) * HEAD)
        out = offs[h] + nt(reads[h], got5[h // 4, h % 4])
        out = out * lax.rsqrt(jnp.mean(out * out, axis=-1, keepdims=True) + epsilon)
        normed[:, part] = (out * gain * silu(gate_ref[:, part].astype(F32))).astype(BF16)
    own.wait()
    for copy in third:
        copy.wait_recv()
    columns = WIDTH // 4
    for k in range(4):
        here = slice(k * columns, (k + 1) * columns)
        mixed_rows[:, here] = nn(normed[...], wall[k].reshape(WIDTH, columns))
    after = (res_ref[...].astype(F32) + mixed_rows[...]).astype(BF16)
    after_ref[...] = after
    wide = after.astype(F32)
    normed[...] = (
        wide * lax.rsqrt(jnp.mean(wide * wide, axis=-1, keepdims=True) + epsilon) * post_ref[...]
    ).astype(BF16)
    rows_copy = send(normed, there, send0.at[2], recv0.at[2], partner)
    routed_ref[0:ROWS, :] = normed[...]
    rows_copy.wait_recv()
    routed_ref[ROWS : 2 * ROWS, :] = there[...]
    for copy in started:
        copy.wait_send()
    for other in range(4):

        @pl.when(other != y)
        def _():
            pltpu.make_async_copy(got1.at[other], got1.at[other], send1.at[other]).wait()


def front(mixed, conv_weight, decay, strength, ids, gate, gain, residual, post, out_weight):
    dma = pltpu.SemaphoreType.DMA
    cut = (2, 4, 2, WIDTH // 16, WIDTH // 4)
    shape = jax.ShapeDtypeStruct((ROWS, WIDTH), BF16)
    return pl.pallas_call(
        front_kernel,
        name="front",
        in_specs=[VM] * 10 + [ANY],
        out_specs=[VM] * 4,
        out_shape=[
            shape, jax.ShapeDtypeStruct((2 * ROWS, WIDTH), BF16),
            jax.ShapeDtypeStruct((2 * ROWS, SENT), BF16),
            jax.ShapeDtypeStruct((2 * ROWS, TOP), F32),
        ],
        scratch_shapes=[
            pltpu.VMEM((ROWS, WIDTH), BF16),
            pltpu.VMEM((16, 2 * WIDTH), BF16),
            pltpu.VMEM((TOP, ROWS), jnp.int32),
            pltpu.VMEM((8 + ROWS, 4 * HEAD), F32),
            pltpu.VMEM((VHEADS, ROWS), F32),
            pltpu.VMEM((BATCH, ROWS, ROWS), F32),
            pltpu.VMEM((BATCH, ROWS, ROWS), F32),
            pltpu.VMEM((VHEADS, 2 * HEAD, HEAD), BF16),
            pltpu.VMEM((VHEADS, ROWS, HEAD), BF16),
            pltpu.VMEM((VHEADS, ROWS, HEAD), F32),
            pltpu.VMEM((4, *cut), BF16),
            pltpu.VMEM((ROWS, WIDTH), BF16),
            pltpu.VMEM((ROWS, WIDTH), F32),
            pltpu.VMEM((4, 4, 2 * HEAD, HEAD), BF16),
            pltpu.VMEM((3, 4, 2 * HEAD, HEAD), BF16),
            pltpu.VMEM((4, 2 * HEAD, HEAD), BF16),
            pltpu.VMEM((8, HEAD + 64, HEAD), BF16),
            pltpu.VMEM((7, HEAD + 64, HEAD), BF16),
            pltpu.VMEM((HEAD + 64, HEAD), BF16),
            pltpu.VMEM((4, HEAD + 64, HEAD), BF16),
            pltpu.VMEM((8, 64, HEAD), BF16),
            pltpu.VMEM((4, HEAD, HEAD), BF16),
            pltpu.VMEM((4, 4, HEAD, HEAD), BF16),
            pltpu.VMEM((4, 4, HEAD, HEAD), BF16),
            dma, dma((3,)), dma((3,)), dma((4,)), dma((4,)), dma((8, 2)), dma((8, 2)),
            dma((4,)), dma((4,)), dma((8,)), dma((8,)), dma((4,)), dma((4,)),
            dma((4, 2)), dma((4, 2)), dma((4, 4, 2)), dma((4, 4, 2)), dma((4, 4, 2)),
            dma((4, 4, 2)),
        ],
        compiler_params=pltpu.CompilerParams(
            collective_id=0, has_side_effects=True, vmem_limit_bytes=56 << 20
        ),
        cost_estimate=pl.CostEstimate(
            flops=30_000_000_000, bytes_accessed=14_000_000, transcendentals=1_500_000
        ),
    )(
        mixed, conv_weight, decay, strength, ids, jnp.asarray(TABLE), gate, gain, residual, post,
        out_weight.reshape(cut),
    )


def distance(group, i):
    dx = lax.rem(i, 4)
    dy = lax.rem(dx + lax.rem(group, 4), 4)
    dz = lax.rem(dx + 2 * (i // 4) + group // 4, 4)
    return dz, dx, dy


LANES = np.arange(SENT)
PEER, INSIDE = LANES // SLOTS, LANES % SLOTS
NEAR = PEER % 8
TABLE = np.stack(
    [
        (NEAR + 2 * (NEAR // 4) + PEER // 32) % 4,
        NEAR % 4,
        (NEAR + PEER // 8) % 4,
        INSIDE // (2 * CAP),
        INSIDE % (2 * CAP) // CAP,
        INSIDE % CAP,
        0 * LANES,
        0 * LANES,
    ]
).astype(np.int32)


def wanted_experts(table_ref, lanes=slice(None)):
    z, x, c, y = (lax.axis_index(a) for a in AXES)
    there = ((table_ref[0:1, lanes] + z) & 3) * 32 + ((table_ref[1:2, lanes] + x) & 3) * 8
    there = there + c * 4 + ((table_ref[2:3, lanes] + y) & 3)
    return 2 * there + table_ref[3:4, lanes]


GROUPS, EACH = 8, 8
BUILT = 2 * EACH * SLOTS


def moe_kernel(
    routed, after, sel, ids_ref, table_ref, switch, router, s_gate, s_up, s_down, gate, up, down,
    out_ref, out_buf, in_buf, back_buf, high, low, total, swap, theirs,
    v_router, v_sgate, v_sup, v_sdown, v_gate, v_up, v_down,
    load_sems, send1, recv1, send2, recv2, send_y, recv_y,
):
    z, x, c, y = (lax.axis_index(a) for a in AXES)
    partner = {"ctx_2": 1 - c}
    barrier = pltpu.get_barrier_semaphore()

    def peer(group, i, sign):
        dz, dx, dy = distance(group, i)
        return {
            "ctx_0": lax.rem(z + 4 + sign * dz, 4),
            "ctx_1": lax.rem(x + 4 + sign * dx, 4),
            "exp": lax.rem(y + 4 + sign * dy, 4),
        }

    def greet(k, _):
        pl.semaphore_signal(
            barrier, inc=1, device_id=peer(k // EACH, lax.rem(k, EACH), 1), device_id_type=MESH
        )
        return 0

    lax.fori_loop(1, PEERS, greet, 0)
    pl.semaphore_signal(barrier, inc=1, device_id=partner, device_id_type=MESH)
    loads = [
        pltpu.make_async_copy(src, dst, load_sems.at[k])
        for k, (src, dst) in enumerate(
            (
                (router, v_router), (s_gate, v_sgate), (s_up, v_sup), (s_down, v_sdown),
                (gate, v_gate), (up, v_up), (down, v_down),
            )
        )
    ]
    for load in loads:
        load.start()

    def build(p):
        lanes = slice(p * BUILT, (p + 1) * BUILT)
        built = tn(sel[:, lanes], routed[...]).astype(BF16)
        out_buf[2 * p * EACH : 2 * (p + 1) * EACH] = built.reshape(2 * EACH, SLOTS, WIDTH)

    build(0)
    pl.semaphore_wait(barrier, PEERS)

    def remote(src, dst, s, r, device):
        return pltpu.make_async_remote_copy(
            src_ref=src, dst_ref=dst, send_sem=s, recv_sem=r, device_id=device, device_id_type=MESH
        )

    def dispatch(group, begin):
        def one(i, _):
            g = group * EACH + i
            remote(
                out_buf.at[g], in_buf.at[g], send1.at[group], recv1.at[group], peer(group, i, 1)
            ).start()
            return 0

        lax.fori_loop(begin, EACH, one, 0)

    def give_back(group, begin):
        def one(i, _):
            g = group * EACH + i
            remote(
                in_buf.at[g], back_buf.at[g], send2.at[group], recv2.at[group], peer(group, i, -1)
            ).start()
            return 0

        lax.fori_loop(begin, EACH, one, 0)

    for p in range(GROUPS // 2):
        if p:
            build(p)
        dispatch(2 * p, 0 if p else 1)
        dispatch(2 * p + 1, 0)
        if p == 0:
            pltpu.make_async_copy(out_buf.at[0], in_buf.at[0], recv1.at[0]).start()

    loads[0].wait()
    logits = nn(routed[...], v_router[...])
    lane = lax.broadcasted_iota(jnp.int32, (2 * ROWS, EXPERTS), 1).astype(F32)
    ids = ids_ref[...]
    hit = ids[:, 0:1] == lane
    for k in range(1, TOP):
        hit = hit | (ids[:, k : k + 1] == lane)
    chosen = jnp.where(hit, jnp.exp(jnp.where(hit, logits, 0.0)), 0.0)
    gates = chosen / jnp.sum(chosen, axis=1, keepdims=True)
    gates_high = gates.astype(BF16)
    gates_low = (gates - gates_high.astype(F32)).astype(BF16)
    for p in range(GROUPS // 2):
        lanes = slice(p * BUILT, (p + 1) * BUILT)
        spread = (
            lax.broadcasted_iota(jnp.int32, (EXPERTS, BUILT), 0) == wanted_experts(table_ref, lanes)
        ).astype(BF16)
        high[p] = nn(gates_high, spread).astype(BF16) * sel[:, lanes]
        low[p] = nn(gates_low, spread).astype(BF16) * sel[:, lanes]

    for load in loads[1:4]:
        load.wait()
    mine = routed[0:ROWS, :]
    hidden = (silu(nn(mine, v_sgate[...])) * nn(mine, v_sup[...])).astype(BF16)
    open_ = jnp.sum(mine.astype(F32) * switch[...].astype(F32), axis=1, keepdims=True)
    total[0:ROWS, :] = after[...].astype(F32) + nn(hidden, v_sdown[...]) / (1.0 + jnp.exp(-open_))
    total[ROWS:, :] = jnp.zeros((ROWS, WIDTH), F32)

    for load in loads[4:]:
        load.wait()

    def serve(group, begin):
        here = pl.ds(group * EACH, EACH)
        pltpu.make_async_copy(in_buf.at[here], in_buf.at[here], recv1.at[group]).wait()
        n = EACH * SLOTS
        rows = in_buf[here].reshape(n, WIDTH)
        inside = lax.rem(lax.broadcasted_iota(jnp.int32, (n, 1), 0), SLOTS)
        result = None
        for e in range(2):
            hidden = silu(nn(rows, v_gate[e])) * nn(rows, v_up[e])
            hidden = jnp.where((inside >= 2 * CAP) == bool(e), hidden, 0.0).astype(BF16)
            part = nn(hidden, v_down[e])
            result = part if result is None else result + part
        in_buf[here] = result.astype(BF16).reshape(EACH, SLOTS, WIDTH)

    serve(0, 1)
    pltpu.make_async_copy(in_buf.at[0], back_buf.at[0], recv2.at[0]).start()
    give_back(0, 1)

    def later(group, _):
        serve(group, 0)
        give_back(group, 0)
        return 0

    lax.fori_loop(1, GROUPS, later, 0)

    for p in range(GROUPS // 2):
        for group in (2 * p, 2 * p + 1):
            here = pl.ds(group * EACH, EACH)
            pltpu.make_async_copy(back_buf.at[here], back_buf.at[here], recv2.at[group]).wait()
        rows = back_buf[2 * p * EACH : 2 * (p + 1) * EACH].reshape(BUILT, WIDTH)
        part = total[ROWS:, :] + nn(high[p, ROWS:, :], rows) + nn(low[p, ROWS:, :], rows)
        if p < GROUPS // 2 - 1:
            total[ROWS:, :] = part
        else:
            theirs[...] = part.astype(BF16)
            last = remote(theirs, swap, send_y, recv_y, partner)
            last.start()
        total[0:ROWS, :] += nn(high[p, 0:ROWS, :], rows) + nn(low[p, 0:ROWS, :], rows)

    last.wait_recv()
    out_ref[...] = (total[0:ROWS, :] + swap[...].astype(F32)).astype(BF16)

    last.wait_send()
    for group in range(GROUPS):
        here = pl.ds(1, EACH - 1) if group == 0 else pl.ds(group * EACH, EACH)
        pltpu.make_async_copy(out_buf.at[here], out_buf.at[here], send1.at[group]).wait()
        pltpu.make_async_copy(in_buf.at[here], in_buf.at[here], send2.at[group]).wait()


def experts(
    routed, after, sel, ids, switch, router, s_gate, s_up, s_down, gate, up, down
):
    dma = pltpu.SemaphoreType.DMA
    vmem = lambda a: pltpu.VMEM(a.shape, a.dtype)
    slabs = pltpu.VMEM((PEERS, SLOTS, WIDTH), BF16)
    weights = (router, s_gate, s_up, s_down, gate, up, down)
    return pl.pallas_call(
        moe_kernel,
        name="experts",
        in_specs=[VM] * 6 + [ANY] * 7,
        out_specs=VM,
        out_shape=jax.ShapeDtypeStruct((ROWS, WIDTH), BF16),
        scratch_shapes=[
            slabs, slabs, slabs,
            pltpu.VMEM((GROUPS // 2, 2 * ROWS, BUILT), BF16),
            pltpu.VMEM((GROUPS // 2, 2 * ROWS, BUILT), BF16),
            pltpu.VMEM((2 * ROWS, WIDTH), F32),
            pltpu.VMEM((ROWS, WIDTH), BF16),
            pltpu.VMEM((ROWS, WIDTH), BF16),
            *(vmem(w) for w in weights),
            dma((7,)), dma((GROUPS,)), dma((GROUPS,)), dma((GROUPS,)), dma((GROUPS,)),
            dma, dma,
        ],
        compiler_params=pltpu.CompilerParams(
            collective_id=1, has_side_effects=True, vmem_limit_bytes=62 << 20
        ),
        cost_estimate=pl.CostEstimate(
            flops=60_000_000_000, bytes_accessed=30_000_000, transcendentals=2_000_000
        ),
    )(routed, after, sel, ids, jnp.asarray(TABLE), switch, *weights)


def local(
    residual, mixed_qkv, output_gate, log_decay, write_strength, conv_weight, norm_gain,
    out_weight, post_gain, router_weight, expert_ids, expert_gate, expert_up, expert_down,
    shared_gate, shared_up, shared_down, shared_switch,
):
    after_mix, routed_in, sel, ids = front(
        mixed_qkv, conv_weight, log_decay.T, write_strength.T, expert_ids.T, output_gate,
        norm_gain.reshape(1, HEAD), residual, post_gain.reshape(1, WIDTH), out_weight,
    )
    return experts(
        routed_in, after_mix, sel, ids, shared_switch.reshape(1, WIDTH), router_weight,
        shared_gate, shared_up, shared_down, expert_gate, expert_up, expert_down,
    )


def solution(mesh):
    finer = Mesh(mesh.devices.reshape(4, 4, 2, mesh.shape["exp"]), AXES)
    rows = P(AXES, None)
    held = P(AXES, None, None)
    placed = (
        rows, rows, rows, rows, rows, P(), P(), P(None, "exp"), P(), P(), rows, held, held, held,
        P(), P(), P(), P(),
    )
    return jax.shard_map(local, mesh=finer, in_specs=placed, out_specs=rows, check_vma=False)
```

```python
import jax
import jax.numpy as jnp
import numpy as np
from jax import lax
from jax.experimental import pallas as pl
from jax.experimental.pallas import tpu as pltpu
from jax.sharding import Mesh
from jax.sharding import PartitionSpec as P

VHEADS = 16
HEAD = 128
ROWS = 128
TOP = 10
CAP = 6
WIDTH = 2048
EXPERTS = 256
AXES = ("ctx_0", "ctx_1", "ctx_2", "exp")
PEERS = 64
SLOTS = 4 * CAP
SENT = PEERS * SLOTS
BATCH = 8
MESH = pl.DeviceIdType.MESH
epsilon = 1e-06
F32 = jnp.float32
BF16 = jnp.bfloat16
VM = pl.BlockSpec(memory_space=pltpu.VMEM)
ANY = pl.BlockSpec(memory_space=pl.ANY)


def nn(a, b):
    return lax.dot_general(a, b, (((1,), (0,)), ((), ())), preferred_element_type=F32)


def nt(a, b):
    return lax.dot_general(a, b, (((1,), (1,)), ((), ())), preferred_element_type=F32)


def tn(a, b):
    return lax.dot_general(a, b, (((0,), (0,)), ((), ())), preferred_element_type=F32)


def silu(v):
    return v / (1.0 + jnp.exp(-v))


def front_kernel(
    mixed, conv, decay_ref, strength_ref, ids_ref, table_ref, gate_ref, gain_ref, res_ref,
    post_ref, weight,
    after_ref, routed_ref, sel_ref, all_ids,
    there, tail, ids_there, pad, cumt, lows, inv, maps, reads, offs, wall, normed, mixed_rows,
    got1, pre1, tot1, got2, pre2, tot2, got3, st4, got4, st5, got5,
    own_sem, send0, recv0, send1, recv1, send2, recv2, send3, recv3, send4, recv4, send5, recv5,
    sendw1, recvw1, sendw2, recvw2, sendw3, recvw3,
):
    z, x, c, y = (lax.axis_index(a) for a in AXES)
    place = 2 * x + c
    spot = (z * 4 + x) * 8 + c * 4 + y
    partner = {"ctx_2": 1 - c}
    barrier = pltpu.get_barrier_semaphore()

    def whole(k):
        return {
            "ctx_0": k // 32, "ctx_1": lax.rem(k // 8, 4), "ctx_2": lax.rem(k // 4, 2),
            "exp": lax.rem(k, 4),
        }

    following, previous = whole(lax.rem(spot + 1, 128)), whole(lax.rem(spot + 127, 128))

    def at(j, axis):
        if axis == "y":
            return {"exp": lax.rem(y + j, 4)}
        if axis == "z":
            return {"ctx_0": lax.rem(z + j, 4)}
        if axis == "x":
            return {"ctx_1": lax.rem(x + j, 4)}
        other = lax.rem(place + j, 8)
        return {"ctx_1": other // 2, "ctx_2": lax.rem(other, 2)}

    for device in (following, previous):
        pl.semaphore_signal(barrier, inc=1, device_id=device, device_id_type=MESH)
    for axis, count in (("y", 4), ("z", 4), ("p", 8)):
        for j in range(1, count):
            pl.semaphore_signal(barrier, inc=1, device_id=at(j, axis), device_id_type=MESH)
    own = pltpu.make_async_copy(weight, wall.at[y], own_sem)
    own.start()
    pl.semaphore_wait(barrier, 15)
    started = []

    def remote(src, dst, s, r, device):
        return pltpu.make_async_remote_copy(
            src_ref=src, dst_ref=dst, send_sem=s, recv_sem=r, device_id=device, device_id_type=MESH
        )

    def send(*args):
        copy = remote(*args)
        copy.start()
        started.append(copy)
        return copy

    last_rows = send(mixed.at[ROWS - 16 : ROWS], tail, send0.at[0], recv0.at[0], following)
    ids_copy = send(ids_ref, ids_there, send0.at[1], recv0.at[1], partner)
    first = []
    for j in range(1, 4):
        for part, quarter in ((0, x), (1, z)):
            first.append(
                send(
                    weight.at[part, quarter, c], wall.at[y, part, quarter, c],
                    sendw1.at[j, part], recvw1.at[j, part], at(j, "y"),
                )
            )

    rows = lax.broadcasted_iota(jnp.int32, (ROWS, ROWS), 0)
    cols = lax.broadcasted_iota(jnp.int32, (ROWS, ROWS), 1)
    causal = rows >= cols
    strict = rows > cols
    ones = causal.astype(F32)
    eye = (rows == cols).astype(F32)
    eye_b = eye.astype(BF16)

    earlier = strict.astype(BF16)
    wanted = wanted_experts(table_ref)
    source, slot = table_ref[4:5, :], table_ref[5:6, :]
    ids_copy.wait_recv()
    for half, held in ((0, ids_ref), (1, ids_there)):
        ids = nt(eye_b, held[...].astype(F32).astype(BF16))
        all_ids[half * ROWS : (half + 1) * ROWS, :] = ids
        aim = jnp.where(source == half, wanted, -1).astype(F32)
        hit = ids[:, 0:1] == aim
        for k in range(1, TOP):
            hit = hit | (ids[:, k : k + 1] == aim)
        marks = hit.astype(F32)
        rank = nn(earlier, marks.astype(BF16))
        sel_ref[half * ROWS : (half + 1) * ROWS, :] = jnp.where(
            rank == slot.astype(F32), marks, 0.0
        ).astype(BF16)

    decay, highest = decay_ref[...], lax.Precision.HIGHEST

    def exact(p, q):
        return lax.dot_general(
            p, q, (((1,), (1,)), ((), ())), precision=highest, preferred_element_type=F32
        )

    cum = exact(ones, decay)
    cumt[...] = exact(decay, ones)
    strength = exact(eye, strength_ref[...])
    lane = lax.broadcasted_iota(jnp.int32, (ROWS, VHEADS), 1)

    def column(table, head):
        return jnp.sum(jnp.where(lane == head, table, 0.0), axis=1, keepdims=True)

    def activated(begin, n):
        here = pl.ds(pl.multiple_of(begin, HEAD), n)
        pad[0:8, 0:n] = jnp.where(spot > 0, tail[8:16, here].astype(F32), 0.0)
        pad[8 : 8 + ROWS, 0:n] = mixed[:, here].astype(F32)
        total = conv[3:4, here] * pad[8 : 8 + ROWS, 0:n]
        for tap in range(3):
            total = total + conv[tap : tap + 1, here] * pad[5 + tap : 5 + tap + ROWS, 0:n]
        return silu(total)

    def unit(a):
        return a * lax.rsqrt(jnp.sum(a * a, axis=-1, keepdims=True) + epsilon)

    last_rows.wait_recv()

    def terms(batch, _):
        groups = [lax.rem(y + 1 + 2 * batch + part, 4) for part in range(2)]
        heads = [4 * groups[i // 4] + i % 4 for i in range(BATCH)]
        n = 2 * HEAD
        queries = [activated(g * n, n) for g in groups]
        keys = [activated(WIDTH // 2 + g * n, n) for g in groups]
        values = [activated(WIDTH + 2 * g * n, 2 * n) for g in groups]
        per_head = []
        for pair in range(BATCH // 2):
            part = slice(pair % 2 * HEAD, (pair % 2 + 1) * HEAD)
            query = unit(queries[pair // 2][:, part]) * HEAD ** (-0.5)
            key = unit(keys[pair // 2][:, part])
            key_b = key.astype(BF16)
            inner = nt(key_b, key_b)
            scores = nt(query.astype(BF16), key_b)
            for i in (2 * pair, 2 * pair + 1):
                d = column(cum, heads[i])
                b = column(strength, heads[i])
                gap = d - cumt[pl.ds(heads[i], 1), :]
                ratios = jnp.where(causal, jnp.exp(jnp.where(causal, gap, 0.0)), 0.0)
                low = jnp.where(strict, ratios * inner, 0.0) * b
                lows[i] = low
                inv[i] = eye - jnp.where((rows >> 1) == (cols >> 1), low, 0.0)
                end = d[ROWS - 1 : ROWS, :]
                decays = jnp.exp(d)
                right = jnp.concatenate(
                    [
                        (b * decays * key).astype(BF16),
                        (b * values[i // 4][:, i % 4 * HEAD : (i % 4 + 1) * HEAD]).astype(BF16),
                    ],
                    axis=1,
                )
                per_head.append(
                    (
                        (scores * ratios).astype(BF16),
                        query * decays,
                        (key * jnp.exp(end - d)).astype(BF16),
                        right,
                        jnp.exp(end) - 1.0,
                    )
                )
        for level in range(1, 7):
            here = (rows >> (level + 1)) == (cols >> (level + 1))
            here = here & ((rows >> level) != (cols >> level))
            for i in range(BATCH):
                now = inv[i]
                now_b = now.astype(BF16)
                off = jnp.where(here, lows[i], 0.0).astype(BF16)
                inv[i] = now - nn(now_b, nn(off, now_b).astype(BF16))
        for i in range(BATCH):
            score, read, end_key, right, less = per_head[i]
            solved = nn(inv[i].astype(BF16), right).astype(BF16)
            carried = tn(solved, end_key)
            maps[heads[i], 0:HEAD, :] = (less * eye - carried[0:HEAD]).astype(BF16)
            maps[heads[i], HEAD : 2 * HEAD, :] = carried[HEAD:].astype(BF16)
            produced = nn(score, solved)
            reads[heads[i]] = (read - produced[:, 0:HEAD]).astype(BF16)
            offs[heads[i]] = produced[:, HEAD:]
        for other in groups:
            four = maps.at[pl.ds(4 * other, 4)]

            @pl.when(other != y)
            def _():
                remote(four, got1.at[y], send1.at[other], recv1.at[y], {"exp": other}).start()

            @pl.when(other == y)
            def _():
                pltpu.make_async_copy(four, got1.at[y], recv1.at[y]).start()

        return 0

    lax.fori_loop(0, VHEADS // BATCH, terms, 0)

    for copy in first:
        copy.wait_recv()

    def spread(k):
        copies = []
        for j in range(1, 4):
            other = lax.rem(y + j, 4)
            for part, quarter, device in ((0, x, at(k, "x")), (1, z, at(k, "z"))):
                held = wall.at[other, part, quarter, c]
                copies.append(
                    send(held, held, sendw2.at[k, j, part], recvw2.at[k, j, part], device)
                )
        return copies

    def across(k):
        copies = []
        for j in range(1, 4):
            other = lax.rem(y + j, 4)
            for part, quarter in ((0, lax.rem(x + 4 - k, 4)), (1, lax.rem(z + 4 - k, 4))):
                held = wall.at[other, part, quarter, c]
                copies.append(
                    send(held, held, sendw3.at[k, j, part], recvw3.at[k, j, part], partner)
                )
        return copies

    second = spread(1) + spread(3)
    third = across(0)

    for m in range(4):
        pltpu.make_async_copy(got1.at[m], got1.at[m], recv1.at[m]).wait()
    for h in range(4):
        run = got1[0, h].astype(F32)
        for m in range(1, 4):
            pre1[m - 1, h] = run.astype(BF16)
            run = run + got1[m, h].astype(F32) + nn(run.astype(BF16), got1[m, h, 0:HEAD, :])
        tot1[h] = run.astype(BF16)

    copies = []
    for j in range(1, 8):
        other = lax.rem(place + j, 8)
        head, half = other // 2, lax.rem(other, 2)
        copies.append(
            send(
                tot1.at[head, 0:HEAD], got2.at[place, 0:HEAD], send2.at[j, 0], recv2.at[j, 0],
                at(j, "p"),
            )
        )
        copies.append(
            send(
                tot1.at[head, pl.ds(pl.multiple_of(HEAD + 64 * half, 64), 64)],
                got2.at[place, HEAD : HEAD + 64],
                send2.at[j, 1], recv2.at[j, 1], at(j, "p"),
            )
        )
    second_last = spread(2)
    got2[place, 0:HEAD, :] = tot1[x, 0:HEAD, :]
    got2[place, HEAD : HEAD + 64, :] = tot1[x, pl.ds(pl.multiple_of(HEAD + 64 * c, 64), 64), :]
    for copy in copies:
        copy.wait_recv()
    run = got2[0].astype(F32)
    for p in range(1, 8):
        pre2[p - 1] = run.astype(BF16)
        run = run + got2[p].astype(F32) + nn(run.astype(BF16), got2[p, 0:HEAD, :])
    tot2[...] = run.astype(BF16)

    copies = []
    for j in range(1, 4):
        copies.append(send(tot2, got3.at[z], send3.at[j], recv3.at[j], at(j, "z")))
    got3[z] = tot2[...]
    for copy in second:
        copy.wait_recv()
    third += across(1) + across(3)
    for copy in copies:
        copy.wait_recv()
    state = jnp.zeros((64, HEAD), F32)
    for k in range(3):
        later = state + got3[k, HEAD:, :].astype(F32) + nn(state.astype(BF16), got3[k, 0:HEAD, :])
        state = jnp.where(k < z, later, state)
    state_b = state.astype(BF16)
    st4[0] = state_b
    for p in range(1, 8):
        st4[p] = (
            state + pre2[p - 1, HEAD:, :].astype(F32) + nn(state_b, pre2[p - 1, 0:HEAD, :])
        ).astype(BF16)

    copies = []
    rows_here = pl.ds(pl.multiple_of(64 * c, 64), 64)
    for j in range(1, 8):
        other = lax.rem(place + j, 8)
        copies.append(
            send(st4.at[other], got4.at[x, rows_here], send4.at[j], recv4.at[j], at(j, "p"))
        )
    got4[x, rows_here, :] = st4[place]
    for copy in second_last:
        copy.wait_recv()
    third += across(2)
    for copy in copies:
        copy.wait_recv()
    for h in range(4):
        begin = got4[h]
        st5[0, h] = begin
        for m in range(1, 4):
            st5[m, h] = (
                begin.astype(F32)
                + pre1[m - 1, h, HEAD:, :].astype(F32)
                + nn(begin, pre1[m - 1, h, 0:HEAD, :])
            ).astype(BF16)

    copies = []
    for j in range(1, 4):
        other = lax.rem(y + j, 4)
        copies.append(send(st5.at[other], got5.at[y], send5.at[j], recv5.at[j], at(j, "y")))
    got5[y] = st5[y]
    own.wait()
    for copy in third:
        copy.wait_recv()

    gain = gain_ref[...]
    columns = WIDTH // 4
    for j in (0, 1, 3, 2):
        member = lax.rem(y + 4 - j, 4)
        if j:
            copies[j - 1].wait_recv()
        four = []
        for i in range(4):
            h = 4 * member + i
            gate_here = gate_ref[:, pl.ds(pl.multiple_of(HEAD * h, HEAD), HEAD)].astype(F32)
            out = offs[h] + nt(reads[h], got5[member, i])
            out = out * lax.rsqrt(jnp.mean(out * out, axis=-1, keepdims=True) + epsilon)
            four.append((out * gain * silu(gate_here)).astype(BF16))
        four = jnp.concatenate(four, axis=1)
        for k in range(4):
            here = slice(k * columns, (k + 1) * columns)
            block = wall[k, member // 2, pl.ds(2 * lax.rem(member, 2), 2)]
            added = nn(four, block.reshape(4 * HEAD, columns))
            mixed_rows[:, here] = mixed_rows[:, here] + added if j else added
    after = (res_ref[...].astype(F32) + mixed_rows[...]).astype(BF16)
    after_ref[...] = after
    wide = after.astype(F32)
    normed[...] = (
        wide * lax.rsqrt(jnp.mean(wide * wide, axis=-1, keepdims=True) + epsilon) * post_ref[...]
    ).astype(BF16)
    rows_copy = send(normed, there, send0.at[2], recv0.at[2], partner)
    routed_ref[0:ROWS, :] = normed[...]
    rows_copy.wait_recv()
    routed_ref[ROWS : 2 * ROWS, :] = there[...]
    for copy in started:
        copy.wait_send()
    for other in range(4):

        @pl.when(other != y)
        def _():
            pltpu.make_async_copy(got1.at[other], got1.at[other], send1.at[other]).wait()


def front(mixed, conv_weight, decay, strength, ids, gate, gain, residual, post, out_weight):
    dma = pltpu.SemaphoreType.DMA
    cut = (2, 4, 2, WIDTH // 16, WIDTH // 4)
    shape = jax.ShapeDtypeStruct((ROWS, WIDTH), BF16)
    return pl.pallas_call(
        front_kernel,
        name="front",
        in_specs=[VM] * 10 + [ANY],
        out_specs=[VM] * 4,
        out_shape=[
            shape, jax.ShapeDtypeStruct((2 * ROWS, WIDTH), BF16),
            jax.ShapeDtypeStruct((2 * ROWS, SENT), BF16),
            jax.ShapeDtypeStruct((2 * ROWS, TOP), F32),
        ],
        scratch_shapes=[
            pltpu.VMEM((ROWS, WIDTH), BF16),
            pltpu.VMEM((16, 2 * WIDTH), BF16),
            pltpu.VMEM((TOP, ROWS), jnp.int32),
            pltpu.VMEM((8 + ROWS, 4 * HEAD), F32),
            pltpu.VMEM((VHEADS, ROWS), F32),
            pltpu.VMEM((BATCH, ROWS, ROWS), F32),
            pltpu.VMEM((BATCH, ROWS, ROWS), F32),
            pltpu.VMEM((VHEADS, 2 * HEAD, HEAD), BF16),
            pltpu.VMEM((VHEADS, ROWS, HEAD), BF16),
            pltpu.VMEM((VHEADS, ROWS, HEAD), F32),
            pltpu.VMEM((4, *cut), BF16),
            pltpu.VMEM((ROWS, WIDTH), BF16),
            pltpu.VMEM((ROWS, WIDTH), F32),
            pltpu.VMEM((4, 4, 2 * HEAD, HEAD), BF16),
            pltpu.VMEM((3, 4, 2 * HEAD, HEAD), BF16),
            pltpu.VMEM((4, 2 * HEAD, HEAD), BF16),
            pltpu.VMEM((8, HEAD + 64, HEAD), BF16),
            pltpu.VMEM((7, HEAD + 64, HEAD), BF16),
            pltpu.VMEM((HEAD + 64, HEAD), BF16),
            pltpu.VMEM((4, HEAD + 64, HEAD), BF16),
            pltpu.VMEM((8, 64, HEAD), BF16),
            pltpu.VMEM((4, HEAD, HEAD), BF16),
            pltpu.VMEM((4, 4, HEAD, HEAD), BF16),
            pltpu.VMEM((4, 4, HEAD, HEAD), BF16),
            dma, dma((3,)), dma((3,)), dma((4,)), dma((4,)), dma((8, 2)), dma((8, 2)),
            dma((4,)), dma((4,)), dma((8,)), dma((8,)), dma((4,)), dma((4,)),
            dma((4, 2)), dma((4, 2)), dma((4, 4, 2)), dma((4, 4, 2)), dma((4, 4, 2)),
            dma((4, 4, 2)),
        ],
        compiler_params=pltpu.CompilerParams(
            collective_id=0, has_side_effects=True, vmem_limit_bytes=56 << 20
        ),
        cost_estimate=pl.CostEstimate(
            flops=30_000_000_000, bytes_accessed=14_000_000, transcendentals=1_500_000
        ),
    )(
        mixed, conv_weight, decay, strength, ids, jnp.asarray(TABLE), gate, gain, residual, post,
        out_weight.reshape(cut),
    )


def distance(group, i):
    dx = lax.rem(i, 4)
    dy = lax.rem(dx + lax.rem(group, 4), 4)
    dz = lax.rem(dx + 2 * (i // 4) + group // 4, 4)
    return dz, dx, dy


LANES = np.arange(SENT)
PEER, INSIDE = LANES // SLOTS, LANES % SLOTS
NEAR = PEER % 8
TABLE = np.stack(
    [
        (NEAR + 2 * (NEAR // 4) + PEER // 32) % 4,
        NEAR % 4,
        (NEAR + PEER // 8) % 4,
        INSIDE // (2 * CAP),
        INSIDE % (2 * CAP) // CAP,
        INSIDE % CAP,
        0 * LANES,
        0 * LANES,
    ]
).astype(np.int32)


def wanted_experts(table_ref, lanes=slice(None)):
    z, x, c, y = (lax.axis_index(a) for a in AXES)
    there = ((table_ref[0:1, lanes] + z) & 3) * 32 + ((table_ref[1:2, lanes] + x) & 3) * 8
    there = there + c * 4 + ((table_ref[2:3, lanes] + y) & 3)
    return 2 * there + table_ref[3:4, lanes]


GROUPS, EACH = 8, 8
BUILT = 2 * EACH * SLOTS


def moe_kernel(
    routed, after, sel, ids_ref, table_ref, switch, router, s_gate, s_up, s_down, gate, up, down,
    out_ref, out_buf, in_buf, back_buf, high, low, total, swap, theirs,
    v_router, v_sgate, v_sup, v_sdown, v_gate, v_up, v_down,
    load_sems, send1, recv1, send2, recv2, send_y, recv_y,
):
    z, x, c, y = (lax.axis_index(a) for a in AXES)
    partner = {"ctx_2": 1 - c}
    barrier = pltpu.get_barrier_semaphore()

    def peer(group, i, sign):
        dz, dx, dy = distance(group, i)
        return {
            "ctx_0": lax.rem(z + 4 + sign * dz, 4),
            "ctx_1": lax.rem(x + 4 + sign * dx, 4),
            "exp": lax.rem(y + 4 + sign * dy, 4),
        }

    def greet(k, _):
        pl.semaphore_signal(
            barrier, inc=1, device_id=peer(k // EACH, lax.rem(k, EACH), 1), device_id_type=MESH
        )
        return 0

    lax.fori_loop(1, PEERS, greet, 0)
    pl.semaphore_signal(barrier, inc=1, device_id=partner, device_id_type=MESH)
    loads = [
        pltpu.make_async_copy(src, dst, load_sems.at[k])
        for k, (src, dst) in enumerate(
            (
                (router, v_router), (s_gate, v_sgate), (s_up, v_sup), (s_down, v_sdown),
                (gate, v_gate), (up, v_up), (down, v_down),
            )
        )
    ]
    for load in loads:
        load.start()

    def build(p):
        lanes = slice(p * BUILT, (p + 1) * BUILT)
        built = tn(sel[:, lanes], routed[...]).astype(BF16)
        out_buf[2 * p * EACH : 2 * (p + 1) * EACH] = built.reshape(2 * EACH, SLOTS, WIDTH)

    build(0)
    pl.semaphore_wait(barrier, PEERS)

    def remote(src, dst, s, r, device):
        return pltpu.make_async_remote_copy(
            src_ref=src, dst_ref=dst, send_sem=s, recv_sem=r, device_id=device, device_id_type=MESH
        )

    def dispatch(group, begin):
        def one(i, _):
            g = group * EACH + i
            remote(
                out_buf.at[g], in_buf.at[g], send1.at[group], recv1.at[group], peer(group, i, 1)
            ).start()
            return 0

        lax.fori_loop(begin, EACH, one, 0)

    def give_back(group, begin):
        def one(i, _):
            g = group * EACH + i
            remote(
                in_buf.at[g], back_buf.at[g], send2.at[group], recv2.at[group], peer(group, i, -1)
            ).start()
            return 0

        lax.fori_loop(begin, EACH, one, 0)

    for p in range(GROUPS // 2):
        if p:
            build(p)
        dispatch(2 * p, 0 if p else 1)
        dispatch(2 * p + 1, 0)
        if p == 0:
            pltpu.make_async_copy(out_buf.at[0], in_buf.at[0], recv1.at[0]).start()

    loads[0].wait()
    logits = nn(routed[...], v_router[...])
    lane = lax.broadcasted_iota(jnp.int32, (2 * ROWS, EXPERTS), 1).astype(F32)
    ids = ids_ref[...]
    hit = ids[:, 0:1] == lane
    for k in range(1, TOP):
        hit = hit | (ids[:, k : k + 1] == lane)
    chosen = jnp.where(hit, jnp.exp(jnp.where(hit, logits, 0.0)), 0.0)
    gates = chosen / jnp.sum(chosen, axis=1, keepdims=True)
    gates_high = gates.astype(BF16)
    gates_low = (gates - gates_high.astype(F32)).astype(BF16)
    for p in range(GROUPS // 2):
        lanes = slice(p * BUILT, (p + 1) * BUILT)
        spread = (
            lax.broadcasted_iota(jnp.int32, (EXPERTS, BUILT), 0) == wanted_experts(table_ref, lanes)
        ).astype(BF16)
        high[p] = nn(gates_high, spread).astype(BF16) * sel[:, lanes]
        low[p] = nn(gates_low, spread).astype(BF16) * sel[:, lanes]

    for load in loads[1:4]:
        load.wait()
    mine = routed[0:ROWS, :]
    hidden = (silu(nn(mine, v_sgate[...])) * nn(mine, v_sup[...])).astype(BF16)
    open_ = jnp.sum(mine.astype(F32) * switch[...].astype(F32), axis=1, keepdims=True)
    total[0:ROWS, :] = after[...].astype(F32) + nn(hidden, v_sdown[...]) / (1.0 + jnp.exp(-open_))
    total[ROWS:, :] = jnp.zeros((ROWS, WIDTH), F32)

    for load in loads[4:]:
        load.wait()

    def serve(group, begin):
        here = pl.ds(group * EACH, EACH)
        pltpu.make_async_copy(in_buf.at[here], in_buf.at[here], recv1.at[group]).wait()
        n = EACH * SLOTS
        rows = in_buf[here].reshape(n, WIDTH)
        inside = lax.rem(lax.broadcasted_iota(jnp.int32, (n, 1), 0), SLOTS)
        result = None
        for e in range(2):
            hidden = silu(nn(rows, v_gate[e])) * nn(rows, v_up[e])
            hidden = jnp.where((inside >= 2 * CAP) == bool(e), hidden, 0.0).astype(BF16)
            part = nn(hidden, v_down[e])
            result = part if result is None else result + part
        in_buf[here] = result.astype(BF16).reshape(EACH, SLOTS, WIDTH)

    serve(0, 1)
    pltpu.make_async_copy(in_buf.at[0], back_buf.at[0], recv2.at[0]).start()
    give_back(0, 1)

    def later(group, _):
        serve(group, 0)
        give_back(group, 0)
        return 0

    lax.fori_loop(1, GROUPS, later, 0)

    for p in range(GROUPS // 2):
        for group in (2 * p, 2 * p + 1):
            here = pl.ds(group * EACH, EACH)
            pltpu.make_async_copy(back_buf.at[here], back_buf.at[here], recv2.at[group]).wait()
        rows = back_buf[2 * p * EACH : 2 * (p + 1) * EACH].reshape(BUILT, WIDTH)
        part = total[ROWS:, :] + nn(high[p, ROWS:, :], rows) + nn(low[p, ROWS:, :], rows)
        if p < GROUPS // 2 - 1:
            total[ROWS:, :] = part
        else:
            theirs[...] = part.astype(BF16)
            last = remote(theirs, swap, send_y, recv_y, partner)
            last.start()
        total[0:ROWS, :] += nn(high[p, 0:ROWS, :], rows) + nn(low[p, 0:ROWS, :], rows)

    last.wait_recv()
    out_ref[...] = (total[0:ROWS, :] + swap[...].astype(F32)).astype(BF16)

    last.wait_send()
    for group in range(GROUPS):
        here = pl.ds(1, EACH - 1) if group == 0 else pl.ds(group * EACH, EACH)
        pltpu.make_async_copy(out_buf.at[here], out_buf.at[here], send1.at[group]).wait()
        pltpu.make_async_copy(in_buf.at[here], in_buf.at[here], send2.at[group]).wait()


def experts(
    routed, after, sel, ids, switch, router, s_gate, s_up, s_down, gate, up, down
):
    dma = pltpu.SemaphoreType.DMA
    vmem = lambda a: pltpu.VMEM(a.shape, a.dtype)
    slabs = pltpu.VMEM((PEERS, SLOTS, WIDTH), BF16)
    weights = (router, s_gate, s_up, s_down, gate, up, down)
    return pl.pallas_call(
        moe_kernel,
        name="experts",
        in_specs=[VM] * 6 + [ANY] * 7,
        out_specs=VM,
        out_shape=jax.ShapeDtypeStruct((ROWS, WIDTH), BF16),
        scratch_shapes=[
            slabs, slabs, slabs,
            pltpu.VMEM((GROUPS // 2, 2 * ROWS, BUILT), BF16),
            pltpu.VMEM((GROUPS // 2, 2 * ROWS, BUILT), BF16),
            pltpu.VMEM((2 * ROWS, WIDTH), F32),
            pltpu.VMEM((ROWS, WIDTH), BF16),
            pltpu.VMEM((ROWS, WIDTH), BF16),
            *(vmem(w) for w in weights),
            dma((7,)), dma((GROUPS,)), dma((GROUPS,)), dma((GROUPS,)), dma((GROUPS,)),
            dma, dma,
        ],
        compiler_params=pltpu.CompilerParams(
            collective_id=1, has_side_effects=True, vmem_limit_bytes=62 << 20
        ),
        cost_estimate=pl.CostEstimate(
            flops=60_000_000_000, bytes_accessed=30_000_000, transcendentals=2_000_000
        ),
    )(routed, after, sel, ids, jnp.asarray(TABLE), switch, *weights)


def local(
    residual, mixed_qkv, output_gate, log_decay, write_strength, conv_weight, norm_gain,
    out_weight, post_gain, router_weight, expert_ids, expert_gate, expert_up, expert_down,
    shared_gate, shared_up, shared_down, shared_switch,
):
    after_mix, routed_in, sel, ids = front(
        mixed_qkv, conv_weight, log_decay.T, write_strength.T, expert_ids.T, output_gate,
        norm_gain.reshape(1, HEAD), residual, post_gain.reshape(1, WIDTH), out_weight,
    )
    return experts(
        routed_in, after_mix, sel, ids, shared_switch, router_weight,
        shared_gate, shared_up, shared_down, expert_gate, expert_up, expert_down,
    )


def solution(mesh):
    finer = Mesh(mesh.devices.reshape(4, 4, 2, mesh.shape["exp"]), AXES)
    rows = P(AXES, None)
    held = P(AXES, None, None)
    placed = (
        rows, rows, rows, rows, rows, P(), P(), P(None, "exp"), P(), P(), rows, held, held, held,
        P(), P(), P(), P(),
    )
    return jax.shard_map(local, mesh=finer, in_specs=placed, out_specs=rows, check_vma=False)
```
